512 devices in a mesh: expert: 64 (over z, x), ffn: 8 (over y, core).
Axes of the slice: x: 4, y: 4, z: 16, core: 2. Of those that a mesh axis runs over, the one named last changes fastest.
Arguments:
- tokens: bfloat16 [8192, 4096], P('expert'), may hold values from -6 to 6
- cotangent: bfloat16 [8192, 4096], P('expert'), may hold values from -6 to 6
- expert_ids: int32 [8192, 1], P('expert'), may hold values from 0 to 7; in each aligned block of 128 rows (0 to 127, 128 to 255, ...) at most 20 rows name the same one
- in_weight: bfloat16 [64, 512, 5120], P('expert', None, 'ffn'), may hold values from -0.09375 to 0.09375
- out_weight: bfloat16 [64, 5120, 512], P('expert', 'ffn'), may hold values from -0.078125 to 0.078125
- width_states: float32 [2, 8, 4096], replicated, may hold values from 76.8 to 768
- hidden_states: float32 [2, 8, 5120], P(None, None, 'ffn'), may hold values from 76.8 to 768
Outputs:
- update_in: bfloat16 [64, 512, 5120], P('expert', None, 'ffn')
- update_out: bfloat16 [64, 5120, 512], P('expert', 'ffn')
The draws below stay inside these ranges and needn't reach their ends.
Inputs may be any that keep to these rules, and one draw needn't show every extreme that they name: `expert_ids`: within each block of 128 consecutive rows at most 20 name the same expert; in some block some expert is named by exactly 20 rows; every expert is named somewhere.
All inputs are finite; a program needn't handle non-finite values.
Results may differ from the reference program's by a relative error of at most 0.0049.
Values may be sent and summed in bfloat16 or wider, within the bound.
A program may use at most 64 MiB of HBM per device.

```python
import math
import jax
import jax.numpy as jnp
import numpy as np
from jax import lax

D = 4096
FF = 5120
GROUP = 8
TOK_DEV = 128
EXPERTS = 8
CAP = 20
TOKENS = 8192
N_EXPERT = 64


def shard_levels(key, dims, pieces, least, high):
    factor_of = 1.0
    for position, parts in pieces:
        steps = jax.random.uniform(jax.random.fold_in(jax.random.fold_in(key, 6), position), (parts,), jnp.float32, least / len(pieces), high / len(pieces))
        factor_of = factor_of * jnp.repeat(jnp.exp(steps), dims[position] // parts).reshape((-1,) + (1,) * (len(dims) - 1 - position))
    return factor_of


def shared_out(key, own, number, rows, number_of, top, most, slope):
    order = jax.random.permutation(key, number_of)
    crowded, common = load_shares(number_of, rows * top, most, slope, True), load_shares(number_of, rows * top, most, slope, False)
    places = jnp.arange(number_of)

    def named(lengths, turn):
        used = int((lengths > 0).sum())
        fixed = max(1, used // 4)
        passed = fixed + (places - fixed + turn * (used - fixed)) % max(1, number_of - fixed)
        return jnp.zeros((number_of,), jnp.int32).at[order[jnp.where(places < fixed, places, passed)]].set(jnp.asarray(lengths, jnp.int32))

    lengths = jnp.where(number % 4 == 0, named(crowded, number // 4), named(common, number - number // 4 - 1))
    mixed = jax.random.permutation(jax.random.fold_in(own, 3), number_of)
    donor, sink = mixed[0:number_of // 2 * 2:2], mixed[1:number_of // 2 * 2:2]
    margin = jnp.minimum(lengths[donor] - 1, most - lengths[sink]) // 2
    margin = jnp.where((donor == order[0]) | (sink == order[0]) | (lengths[sink] == 0), 0, jnp.maximum(margin, 0))
    passed = jax.random.randint(jax.random.fold_in(own, 4), (number_of // 2,), 0, 1 << 20) % (margin + 1)
    lengths = lengths.at[donor].add(-passed).at[sink].add(passed)
    members = jnp.searchsorted(jnp.cumsum(lengths), jnp.arange(rows * top), side="right").astype(jnp.int32)
    listing = members.reshape(top, rows).T
    listing = listing[jax.random.permutation(jax.random.fold_in(own, 1), rows)]
    turn = jax.random.randint(jax.random.fold_in(own, 2), (rows, 1), 0, top)
    return jnp.take_along_axis(listing, (jnp.arange(top)[None, :] + turn) % top, axis=1)


def load_shares(amount, total, most, skew, full):
    weights = [(1 << 20) // math.isqrt(grade ** skew) + 1 for grade in range(1, amount + 1)]
    largest = most if full else min(most, max(-(-total // amount), total * weights[0] // sum(weights)))
    least = 1 if total - largest >= amount - 1 else 0
    given, surplus = [largest] + [least] * (amount - 1), total - largest - least * (amount - 1)
    while surplus > 0:
        movable = [i for i in range(1, amount) if given[i] < largest] or [i for i in range(1, amount) if given[i] < most]
        pool, left = sum([weights[i] for i in movable]), surplus
        for i in movable:
            more = min(most - given[i], max(1, left * weights[i] // pool), surplus)
            given[i] = given[i] + more
            surplus = surplus - more
    return np.array(given)


def gaussian(own_key, dims, scale, bound, pieces=(), kind=jnp.bfloat16):
    drawn = scale * jax.random.normal(own_key, dims, jnp.float32)
    if pieces:
        drawn = drawn * shard_levels(own_key, dims, pieces, -0.22, 0.18)
    return jnp.clip(drawn, -bound, bound).astype(kind)


def setup_inputs(seed: int = 0) -> dict:
    arg_keys = jax.random.split(jax.random.key(seed), 8)
    tokens = gaussian(arg_keys[0], (TOKENS, D), 1.0, 6.0, ((0, 64),))
    cotangent = gaussian(arg_keys[1], (TOKENS, D), 1.0, 6.0, ((0, 64),))
    expert_ids_keys = jax.random.split(jax.random.fold_in(arg_keys[2], 1), TOKENS // TOK_DEV)
    expert_ids_turns = jax.random.permutation(jax.random.fold_in(arg_keys[2], 3), TOKENS // TOK_DEV)
    expert_ids = jax.vmap(lambda own, number: shared_out(jax.random.fold_in(arg_keys[2], 2), own, number, TOK_DEV, EXPERTS, 1, CAP, 2))(expert_ids_keys, expert_ids_turns).reshape((TOKENS, 1))
    in_weight = gaussian(arg_keys[3], (EXPERTS * GROUP, D // GROUP, FF), D ** -0.5, 0.09375, ((0, 64), (2, 8)))
    out_weight = gaussian(arg_keys[4], (EXPERTS * GROUP, FF, D // GROUP), FF ** -0.5, 0.078125, ((0, 64), (1, 8)))
    width_states = jnp.clip(jnp.exp(jax.random.uniform(arg_keys[5], (2, EXPERTS, D), jnp.float32, math.log(76.8), math.log(768.0))), 76.8, 768.0)
    hidden_states = jnp.clip(jnp.exp(math.log(768.0) - 2.3025851 * jax.random.uniform(arg_keys[6], (2, EXPERTS, FF), jnp.float32) ** shard_levels(arg_keys[6], (2, EXPERTS, FF), ((2, 8),), -0.2, 0.2)), 76.8, 768.0)
    return dict(tokens=tokens, cotangent=cotangent, expert_ids=expert_ids, in_weight=in_weight, out_weight=out_weight, width_states=width_states, hidden_states=hidden_states)


DECAY_RATE = 0.9
EPS_ONE = 1e-30
ROOT_COEF = math.sqrt(2.0 / math.pi)
CUBIC_COEF = 0.044715

def gelu_pair(inputs):
    inner = ROOT_COEF * (inputs + CUBIC_COEF * inputs * inputs * inputs)
    tangent = jnp.tanh(inner)
    act_value = 0.5 * inputs * (1.0 + tangent)
    act_slope = 0.5 * (1.0 + tangent) + 0.5 * inputs * (1.0 - tangent * tangent) * ROOT_COEF * (1.0 + 3.0 * CUBIC_COEF * inputs * inputs)
    return (act_value, act_slope)

def factored(grad, row_prev, col_prev):
    squares = grad * grad + EPS_ONE
    row_factor = DECAY_RATE * row_prev + (1.0 - DECAY_RATE) * lax.optimization_barrier(jnp.mean(squares, axis=1))
    col_factor = DECAY_RATE * col_prev + (1.0 - DECAY_RATE) * lax.optimization_barrier(jnp.mean(squares, axis=0))
    scale_factor = row_factor[:, None] * col_factor[None, :] / jnp.mean(row_factor)
    update = grad * lax.rsqrt(scale_factor)
    clip_ratio = jnp.sqrt(jnp.mean(update * update))
    return (update / jnp.maximum(1.0, clip_ratio)).astype(jnp.bfloat16)

def reference(tokens, cotangent, expert_ids, in_weight, out_weight, width_states, hidden_states):
    route_ids = expert_ids[:, 0].reshape(N_EXPERT, TOK_DEV)
    onehot = (route_ids[:, :, None] == jnp.arange(EXPERTS, dtype=jnp.int32)[None, None, :]).astype(jnp.int32)
    before = jnp.cumsum(onehot, axis=1) - onehot
    slot_index = lax.optimization_barrier(jnp.sum(before * onehot, axis=2))
    source = jnp.arange(N_EXPERT, dtype=jnp.int32)[:, None]
    target = (source * CAP + slot_index).reshape(-1).astype(jnp.int32)
    flat_ids = route_ids.reshape(-1)
    token_index = jnp.arange(TOKENS, dtype=jnp.int32)
    in_all = in_weight.reshape(EXPERTS, D, FF)
    out_all = out_weight.reshape(EXPERTS, GROUP, FF, D // GROUP).transpose(0, 2, 1, 3).reshape(EXPERTS, FF, D)

    def one_expert(expert):
        place_index = jnp.where(flat_ids == expert, target, N_EXPERT * CAP).astype(jnp.int32)
        chosen = jnp.full((N_EXPERT * CAP,), TOKENS, jnp.int32).at[place_index].set(token_index, mode='drop')
        is_valid = chosen < TOKENS
        safe_index = jnp.minimum(chosen, TOKENS - 1).astype(jnp.int32)
        expert_tokens = tokens[safe_index] * is_valid[:, None].astype(tokens.dtype)
        expert_cotangent = cotangent[safe_index] * is_valid[:, None].astype(cotangent.dtype)
        in_one = in_all[expert]
        out_one = out_all[expert]
        pre_act = jnp.dot(expert_tokens, in_one, preferred_element_type=jnp.float32)
        back_act = jnp.dot(expert_cotangent, out_one.T, preferred_element_type=jnp.float32)
        act_value, act_slope = gelu_pair(pre_act)
        hidden = act_value.astype(jnp.bfloat16)
        pre_grad = (back_act * act_slope).astype(jnp.bfloat16)
        grad_in = jnp.dot(expert_tokens.T, pre_grad, preferred_element_type=jnp.float32)
        grad_out = jnp.dot(hidden.T, expert_cotangent, preferred_element_type=jnp.float32)
        upd_in = factored(grad_in, width_states[0, expert], hidden_states[0, expert])
        upd_out = factored(grad_out, hidden_states[1, expert], width_states[1, expert])
        return (upd_in, upd_out)
    upd_in, upd_out = lax.map(one_expert, jnp.arange(EXPERTS, dtype=jnp.int32))
    update_in = upd_in.reshape(EXPERTS * GROUP, D // GROUP, FF)
    update_out = upd_out.reshape(EXPERTS, FF, GROUP, D // GROUP).transpose(0, 2, 1, 3).reshape(EXPERTS * GROUP, FF, D // GROUP)
    return (update_in, update_out)
```

```python
import math

import jax
import jax.numpy as jnp
from jax import lax
from jax.experimental import pallas as pl
from jax.experimental.pallas import tpu as pltpu
from jax.sharding import PartitionSpec as P

D = 4096
FF = 5120
GROUP = 8
EXPERTS = 8
FFN = 8
CAP = 20
BLK = D // GROUP
HID = FF // FFN
TOK = 128
ROWS = GROUP * CAP
PIECES = 8

DECAY_RATE = 0.9
EPS_ONE = 1e-30
ROOT_COEF = math.sqrt(2.0 / math.pi)
CUBIC_COEF = 0.044715

MESH = pl.DeviceIdType.MESH
F32 = jnp.float32
BF16 = jnp.bfloat16
NT = (((1,), (1,)), ((), ()))
TN = (((0,), (0,)), ((), ()))


def gelu_pair(inputs):
    inner = ROOT_COEF * (inputs + CUBIC_COEF * inputs * inputs * inputs)
    tangent = jnp.tanh(inner)
    act_value = 0.5 * inputs * (1.0 + tangent)
    act_slope = 0.5 * (1.0 + tangent) + 0.5 * inputs * (1.0 - tangent * tangent) * ROOT_COEF * (
        1.0 + 3.0 * CUBIC_COEF * inputs * inputs
    )
    return (act_value, act_slope)


def iota(shape, dim):
    return lax.broadcasted_iota(jnp.int32, shape, dim)


def kernel(
    ids_ref, tok_ref, cot_ref, win_ref, wout_ref, ws_ref, hs_ref,
    uin_ref, uout_ref,
    chunk_s, chunk_r, xall, part_s, part_r, acc, hp, gin, gout,
    lane_in, lane_out, stat_h, stat_w, norm_g, norm_f,
    a2a_ss, a2a_rs, ring_ss, ring_rs, rs_ss, rs_rs, ag_ss, ag_rs,
    sh_ss, sh_rs, sw_ss, sw_rs, ng_ss, ng_rs, nf_ss, nf_rs,
):
    p = lax.axis_index("expert")
    f = lax.axis_index("ffn")
    e = p // GROUP
    i = p % GROUP
    y = f // 2
    core = f % 2

    def turn(value, n):
        return lax.rem(value, n)

    def chunk_of(ff):
        return turn(ff + 2 * GROUP - i - e, GROUP)

    mine = chunk_of(f)
    f_pair = y * 2 + (1 - core)
    f_up = turn(y + 1, 4) * 2 + core
    f_dn = turn(y + 3, 4) * 2 + core
    f_op = turn(y + 2, 4) * 2 + core

    def pair_of(ff):
        return (ff // 2) * 2 + (1 - ff % 2)

    barrier = pltpu.get_barrier_semaphore()
    for q in range(EXPERTS):
        source = q * GROUP + mine

        @pl.when(source != p)
        def _():
            pl.semaphore_signal(barrier, inc=1, device_id=(source, f), device_id_type=MESH)

    for k in range(1, GROUP):
        pl.semaphore_signal(
            barrier, inc=1, device_id=(e * GROUP + turn(i + k, GROUP), f), device_id_type=MESH
        )
        pl.semaphore_signal(barrier, inc=1, device_id=(p, turn(f + k, FFN)), device_id_type=MESH)

    ids = ids_ref[...]
    onehot = iota((EXPERTS, TOK), 0) == ids
    earlier = jnp.where(iota((TOK, TOK), 0) < iota((TOK, TOK), 1), 1.0, 0.0).astype(BF16)
    before = jnp.dot(
        jnp.where(onehot, 1.0, 0.0).astype(BF16), earlier, preferred_element_type=F32
    )
    slot = jnp.sum(jnp.where(onehot, before, 0.0), axis=0, keepdims=True).astype(jnp.int32)
    pieces_row = iota((ROWS, PIECES * TOK), 0) - CAP * (iota((ROWS, PIECES * TOK), 1) // TOK)

    def build(expert, carry):
        place = jnp.where(ids == expert, slot, -ROWS * 2)
        place = jnp.concatenate([place] * PIECES, axis=1)
        select = jnp.where(pieces_row == place, 1.0, 0.0).astype(BF16)
        offset = turn(f + 2 * GROUP - expert - i, GROUP) * BLK
        parts = []
        for ref in (tok_ref, cot_ref):
            for g in range(4):
                parts.append(ref[:, pl.ds(pl.multiple_of(offset + g * 128, 128), 128)])
        chunk_s[expert] = jnp.dot(
            select, jnp.concatenate(parts, axis=0), preferred_element_type=F32
        ).astype(BF16)
        return carry

    lax.fori_loop(0, EXPERTS, build, 0)

    pl.semaphore_wait(barrier, EXPERTS + 2 * (GROUP - 1) - jnp.where(mine == i, 1, 0))

    def routed(expert):
        target = expert * GROUP + turn(f + 2 * GROUP - expert - i, GROUP)
        copy = pltpu.make_async_remote_copy(
            src_ref=chunk_s.at[expert], dst_ref=chunk_r.at[e],
            send_sem=a2a_ss.at[expert], recv_sem=a2a_rs.at[e],
            device_id=(target, f), device_id_type=MESH,
        )
        return target, copy

    for k in range(EXPERTS):
        target, copy = routed(turn(e + 4 + k, EXPERTS))

        @pl.when(target != p)
        def _():
            copy.start()

        @pl.when(target == p)
        def _():
            chunk_r[e] = chunk_s[e]

    def landed(q):
        return pltpu.make_async_remote_copy(
            src_ref=chunk_s.at[q], dst_ref=chunk_r.at[q],
            send_sem=a2a_ss.at[q], recv_sem=a2a_rs.at[q],
            device_id=(p, f), device_id_type=MESH,
        )

    for q in range(EXPERTS):
        @pl.when(q * GROUP + mine != p)
        def _():
            landed(q).wait_recv()

    received = chunk_r[...].reshape(EXPERTS * ROWS, 128)
    row_of = iota((ROWS, EXPERTS * ROWS), 0)
    source_of = lax.shift_right_logical(row_of * 3277, 16)
    gap = iota((ROWS, EXPERTS * ROWS), 1) - (ROWS - CAP) * source_of - row_of
    for piece in range(PIECES):
        select = jnp.where(gap == CAP * piece, 1.0, 0.0).astype(BF16)
        xall[mine, :, piece * 128 : (piece + 1) * 128] = jnp.dot(
            select, received, preferred_element_type=F32
        ).astype(BF16)

    def ring(c, start, size, target, index):
        rows = pl.ds(start, size)
        return pltpu.make_async_remote_copy(
            src_ref=xall.at[c, rows], dst_ref=xall.at[c, rows],
            send_sem=ring_ss.at[index], recv_sem=ring_rs.at[index],
            device_id=(p, target), device_id_type=MESH,
        )

    half = ROWS // 2
    c_pair, c_up, c_dn, c_op = chunk_of(f_pair), chunk_of(f_up), chunk_of(f_dn), chunk_of(f_op)
    to_up = ring(mine, 0, ROWS, f_up, 0)
    to_dn = ring(mine, 0, ROWS, f_dn, 1)
    to_pair = ring(mine, 0, ROWS, f_pair, 2)
    on_up = ring(c_dn, 0, half, f_up, 3)
    on_dn = ring(c_up, half, half, f_dn, 4)
    pair_dn = ring(c_dn, 0, ROWS, f_pair, 5)
    pair_up = ring(c_up, 0, ROWS, f_pair, 6)
    pair_op_a = ring(c_op, 0, half, f_pair, 7)
    pair_op_b = ring(c_op, half, half, f_pair, 8)
    sent = [to_up, to_dn, to_pair, on_up, on_dn, pair_dn, pair_up, pair_op_a, pair_op_b]

    def partial_copy(c):
        return pltpu.make_async_remote_copy(
            src_ref=part_s.at[c], dst_ref=part_r.at[i],
            send_sem=rs_ss.at[c], recv_sem=rs_rs.at[i],
            device_id=(e * GROUP + c, f), device_id_type=MESH,
        )

    def partial_landed(d):
        return pltpu.make_async_remote_copy(
            src_ref=part_s.at[d], dst_ref=part_r.at[d],
            send_sem=rs_ss.at[d], recv_sem=rs_rs.at[d],
            device_id=(e * GROUP + d, f), device_id_type=MESH,
        )

    def partials(c):
        pre = jnp.dot(xall[c, :, :BLK], win_ref[...], preferred_element_type=F32)
        back = lax.dot_general(xall[c, :, BLK:], wout_ref[...], NT, preferred_element_type=F32)

        @pl.when(c == i)
        def _():
            acc[:, :HID] = pre
            acc[:, HID:] = back

        @pl.when(c != i)
        def _():
            part_s[c, :, :HID] = pre.astype(BF16)
            part_s[c, :, HID:] = back.astype(BF16)
            partial_copy(c).start()

    to_up.start()
    to_dn.start()
    to_pair.start()
    partials(mine)
    ring(c_pair, 0, ROWS, f_pair, 2).wait_recv()
    partials(c_pair)
    ring(c_dn, 0, ROWS, f_dn, 0).wait_recv()
    on_up.start()
    pair_dn.start()
    ring(c_up, 0, ROWS, f_up, 1).wait_recv()
    on_dn.start()
    pair_up.start()
    partials(c_dn)
    partials(c_up)
    ring(chunk_of(pair_of(f_dn)), 0, ROWS, f_pair, 5).wait_recv()
    partials(chunk_of(pair_of(f_dn)))
    ring(c_op, 0, half, f_dn, 3).wait_recv()
    pair_op_a.start()
    ring(c_op, half, half, f_up, 4).wait_recv()
    pair_op_b.start()
    ring(chunk_of(pair_of(f_up)), 0, ROWS, f_pair, 6).wait_recv()
    partials(chunk_of(pair_of(f_up)))
    partials(c_op)
    c_last = chunk_of(pair_of(f_op))
    ring(c_last, 0, half, f_pair, 7).wait_recv()
    ring(c_last, half, half, f_pair, 8).wait_recv()
    partials(c_last)

    for k in range(1, GROUP):
        d = turn(i + k, GROUP)
        partial_landed(d).wait_recv()
        acc[...] += part_r[d].astype(F32)

    def activate(block, carry):
        rows = pl.ds(pl.multiple_of(block * 16, 16), 16)
        act_value, act_slope = gelu_pair(acc[rows, :HID])
        hp[i, rows, :HID] = act_value.astype(BF16)
        hp[i, rows, HID:] = (acc[rows, HID:] * act_slope).astype(BF16)
        return carry

    lax.fori_loop(0, ROWS // 16, activate, 0)

    def finished(c, target):
        return pltpu.make_async_remote_copy(
            src_ref=hp.at[c], dst_ref=hp.at[c],
            send_sem=ag_ss.at[target], recv_sem=ag_rs.at[c],
            device_id=(e * GROUP + target, f), device_id_type=MESH,
        )

    for k in range(1, GROUP):
        finished(i, turn(i + k, GROUP)).start()

    for k in range(GROUP):
        d = turn(i + k, GROUP)
        if k:
            finished(d, d).wait_recv()
        add_in = lax.dot_general(
            xall[d, :, :BLK], hp[d, :, HID:], TN, preferred_element_type=F32
        )
        add_out = lax.dot_general(
            hp[d, :, :HID], xall[d, :, BLK:], TN, preferred_element_type=F32
        )
        if k:
            gin[...] += add_in
            gout[...] += add_out
        else:
            gin[...] = add_in
            gout[...] = add_out

    def squares(ref, lanes, width, rows):
        def step(block, total):
            here = pl.ds(pl.multiple_of(block * 32, 32), 32)
            value = ref[here, :]
            value = value * value + EPS_ONE
            folded = value[:, :128]
            for g in range(1, width // 128):
                folded = folded + value[:, g * 128 : (g + 1) * 128]
            lanes[here, :] = folded
            return total + jnp.sum(value.reshape(4, 8, width), axis=0)

        total = lax.fori_loop(0, rows // 32, step, jnp.zeros((8, width), F32))
        return jnp.sum(total, axis=0, keepdims=True), jnp.sum(lanes[...].T, axis=0, keepdims=True)

    cols_in, rows_in = squares(gin, lane_in, HID, BLK)
    cols_out, rows_out = squares(gout, lane_out, BLK, HID)
    hidden_prev = hs_ref[:, pl.ds(e, 1), :]
    width_prev = ws_ref[:, pl.ds(e, 1), pl.ds(pl.multiple_of(i * BLK, BLK), BLK)]
    hidden_sum = jnp.sum(hidden_prev[1], axis=1, keepdims=True)
    stat_h[i] = jnp.concatenate([cols_in, rows_out, jnp.zeros((6, HID), F32)], axis=0)
    stat_w[f] = jnp.concatenate(
        [rows_in, cols_out, jnp.broadcast_to(hidden_sum, (6, BLK))], axis=0
    )

    def exchange(buf, own, ssem, rsem, device):
        copies = []
        for k in range(1, 8):
            d = turn(own + k, 8)
            copies.append((
                pltpu.make_async_remote_copy(
                    src_ref=buf.at[own], dst_ref=buf.at[own],
                    send_sem=ssem.at[d], recv_sem=rsem.at[own],
                    device_id=device(d), device_id_type=MESH,
                ),
                pltpu.make_async_remote_copy(
                    src_ref=buf.at[d], dst_ref=buf.at[d],
                    send_sem=ssem.at[d], recv_sem=rsem.at[d],
                    device_id=device(d), device_id_type=MESH,
                ),
            ))
        return copies

    def in_group(d):
        return (e * GROUP + d, f)

    def in_ffn(d):
        return (p, d)

    over_group = exchange(stat_h, i, sh_ss, sh_rs, in_group)
    over_ffn = exchange(stat_w, f, sw_ss, sw_rs, in_ffn)
    for start, _ in over_group + over_ffn:
        start.start()
    for _, arrival in over_group + over_ffn:
        arrival.wait_recv()
    sum_h = jnp.sum(stat_h[...], axis=0)
    sum_w = jnp.sum(stat_w[...], axis=0)

    cols_in = DECAY_RATE * hidden_prev[0] + (1.0 - DECAY_RATE) * sum_h[0:1] / D
    rows_out = DECAY_RATE * hidden_prev[1] + (1.0 - DECAY_RATE) * sum_h[1:2] / D
    rows_in = DECAY_RATE * width_prev[0] + (1.0 - DECAY_RATE) * sum_w[0:1] / FF
    cols_out = DECAY_RATE * width_prev[1] + (1.0 - DECAY_RATE) * sum_w[1:2] / FF
    lane_in[...] = jnp.broadcast_to(lax.rsqrt(rows_in), (128, BLK)).T
    lane_out[...] = jnp.broadcast_to(lax.rsqrt(rows_out), (128, HID)).T
    scale_in = lax.rsqrt(cols_in)
    scale_out = lax.rsqrt(cols_out)

    def scaled(ref, lanes, scale, width, rows):
        def step(block, total):
            here = pl.ds(pl.multiple_of(block * 32, 32), 32)
            factor = lanes[here, :]
            for g in range(width // 128):
                cols = slice(g * 128, (g + 1) * 128)
                value = ref[here, cols] * factor * scale[:, cols]
                ref[here, cols] = value
                total = total + jnp.sum((value * value).reshape(4, 8, 128), axis=0)
            return total

        total = lax.fori_loop(0, rows // 32, step, jnp.zeros((8, 128), F32))
        return jnp.sum(total, axis=0, keepdims=True)

    norm_in = scaled(gin, lane_in, scale_in, HID, BLK)
    norm_out = scaled(gout, lane_out, scale_out, BLK, HID)

    def fold(row):
        total = row[:, :128]
        for g in range(1, row.shape[1] // 128):
            total = total + row[:, g * 128 : (g + 1) * 128]
        return total

    norm_g[i] = jnp.concatenate(
        [norm_in, norm_out, fold(sum_w[0:1]), fold(sum_w[1:2]), jnp.zeros((4, 128), F32)], axis=0
    )
    group_norms = exchange(norm_g, i, ng_ss, ng_rs, in_group)
    for start, _ in group_norms:
        start.start()
    for _, arrival in group_norms:
        arrival.wait_recv()
    group_sum = jnp.sum(norm_g[...], axis=0)
    norm_f[f] = group_sum
    ffn_norms = exchange(norm_f, f, nf_ss, nf_rs, in_ffn)
    for start, _ in ffn_norms:
        start.start()
    for _, arrival in ffn_norms:
        arrival.wait_recv()
    norm_sum = jnp.sum(jnp.sum(norm_f[...], axis=0), axis=1, keepdims=True)
    totals = jnp.sum(group_sum, axis=1, keepdims=True)

    whole_count = float(D) * float(FF)
    width_mean = jnp.sum(ws_ref[0, pl.ds(e, 1), :], axis=1, keepdims=True) / D
    mean_in = DECAY_RATE * width_mean + (1.0 - DECAY_RATE) * totals[2:3] / whole_count
    mean_out = (
        DECAY_RATE * sum_w[2:3, 0:1] / FF + (1.0 - DECAY_RATE) * totals[3:4] / whole_count
    )
    def last_factor(mean, norm):
        return jnp.sqrt(mean) / jnp.maximum(1.0, jnp.sqrt(mean * (norm / whole_count)))

    factor_in = last_factor(mean_in, norm_sum[0:1])
    factor_out = last_factor(mean_out, norm_sum[1:2])

    def store_in(block, carry):
        here = pl.ds(pl.multiple_of(block * 32, 32), 32)
        uin_ref[here, :] = (gin[here, :] * factor_in).astype(BF16)
        return carry

    def store_out(block, carry):
        here = pl.ds(pl.multiple_of(block * 32, 32), 32)
        uout_ref[here, :] = (gout[here, :] * factor_out).astype(BF16)
        return carry

    lax.fori_loop(0, BLK // 32, store_in, 0)
    lax.fori_loop(0, HID // 32, store_out, 0)

    for q in range(EXPERTS):
        target, copy = routed(q)

        @pl.when(target != p)
        def _():
            copy.wait_send()

    for copy in sent:
        copy.wait_send()
    for k in range(1, GROUP):
        partial_copy(turn(i + k, GROUP)).wait_send()
        finished(i, turn(i + k, GROUP)).wait_send()
    for start, _ in over_group + over_ffn + group_norms + ffn_norms:
        start.wait_send()


def shards(tokens, cotangent, expert_ids, in_weight, out_weight, width_states, hidden_states):
    vmem = pl.BlockSpec(memory_space=pltpu.VMEM)
    dma8 = pltpu.SemaphoreType.DMA((8,))
    update_in, update_out = pl.pallas_call(
        kernel,
        out_shape=(
            jax.ShapeDtypeStruct((BLK, HID), BF16),
            jax.ShapeDtypeStruct((HID, BLK), BF16),
        ),
        in_specs=[vmem] * 7,
        out_specs=(vmem, vmem),
        scratch_shapes=[
            pltpu.VMEM((EXPERTS, ROWS, 128), BF16),
            pltpu.VMEM((EXPERTS, ROWS, 128), BF16),
            pltpu.VMEM((GROUP, ROWS, 2 * BLK), BF16),
            pltpu.VMEM((GROUP, ROWS, 2 * HID), BF16),
            pltpu.VMEM((GROUP, ROWS, 2 * HID), BF16),
            pltpu.VMEM((ROWS, 2 * HID), F32),
            pltpu.VMEM((GROUP, ROWS, 2 * HID), BF16),
            pltpu.VMEM((BLK, HID), F32),
            pltpu.VMEM((HID, BLK), F32),
            pltpu.VMEM((BLK, 128), F32),
            pltpu.VMEM((HID, 128), F32),
            pltpu.VMEM((GROUP, 8, HID), F32),
            pltpu.VMEM((FFN, 8, BLK), F32),
            pltpu.VMEM((GROUP, 8, 128), F32),
            pltpu.VMEM((FFN, 8, 128), F32),
            dma8, dma8,
            pltpu.SemaphoreType.DMA((9,)), pltpu.SemaphoreType.DMA((9,)),
            dma8, dma8, dma8, dma8, dma8, dma8, dma8, dma8, dma8, dma8, dma8, dma8,
        ],
        compiler_params=pltpu.CompilerParams(
            collective_id=0, has_side_effects=True, vmem_limit_bytes=56 * 1024 * 1024
        ),
        name="switch_update",
    )(
        expert_ids.reshape(1, TOK), tokens, cotangent, in_weight[0], out_weight[0],
        width_states, hidden_states,
    )
    return (update_in[None], update_out[None])


def solution(mesh):
    return jax.shard_map(
        shards,
        mesh=mesh,
        in_specs=(
            P("expert", None),
            P("expert", None),
            P("expert", None),
            P("expert", None, "ffn"),
            P("expert", "ffn", None),
            P(),
            P(None, None, "ffn"),
        ),
        out_specs=(P("expert", None, "ffn"), P("expert", "ffn", None)),
        check_vma=False,
    )
```

```python
import math

import jax
import jax.numpy as jnp
from jax import lax
from jax.experimental import pallas as pl
from jax.experimental.pallas import tpu as pltpu
from jax.sharding import PartitionSpec as P

D = 4096
FF = 5120
GROUP = 8
EXPERTS = 8
FFN = 8
CAP = 20
BLK = D // GROUP
HID = FF // FFN
TOK = 128
ROWS = GROUP * CAP
PIECES = 8

DECAY_RATE = 0.9
EPS_ONE = 1e-30
ROOT_COEF = math.sqrt(2.0 / math.pi)
CUBIC_COEF = 0.044715

MESH = pl.DeviceIdType.MESH
F32 = jnp.float32
BF16 = jnp.bfloat16
NT = (((1,), (1,)), ((), ()))
TN = (((0,), (0,)), ((), ()))


def gelu_pair(inputs):
    inner = ROOT_COEF * (inputs + CUBIC_COEF * inputs * inputs * inputs)
    tangent = jnp.tanh(inner)
    act_value = 0.5 * inputs * (1.0 + tangent)
    act_slope = 0.5 * (1.0 + tangent) + 0.5 * inputs * (1.0 - tangent * tangent) * ROOT_COEF * (
        1.0 + 3.0 * CUBIC_COEF * inputs * inputs
    )
    return (act_value, act_slope)


def iota(shape, dim):
    return lax.broadcasted_iota(jnp.int32, shape, dim)


def kernel(
    ids_ref, tok_ref, cot_ref, win_ref, wout_ref, ws_ref, hs_ref,
    uin_ref, uout_ref,
    chunk_s, chunk_r, xall, part_s, relay_r, next_r, pair_r, work, acc, hp, gin, gout,
    lane_in, lane_out, stat_h, stat_w, norm_g, norm_f,
    a2a_ss, a2a_rs, ring_ss, ring_rs, rel_ss, rel_rs, nex_ss, nex_rs, par_ss, par_rs, ag_ss, ag_rs,
    sh_ss, sh_rs, sw_ss, sw_rs, ng_ss, ng_rs, nf_ss, nf_rs,
):
    p = lax.axis_index("expert")
    f = lax.axis_index("ffn")
    e = p // GROUP
    i = p % GROUP
    y = f // 2
    core = f % 2

    def turn(value, n):
        return lax.rem(value, n)

    def flip(value, mask):
        for bit in (1, 2, 4):
            if mask & bit:
                value = value + bit * (1 - 2 * turn(value // bit, 2))
        return value

    def xor(*values):
        total = 0
        for bit in (1, 2, 4):
            total = total + bit * turn(sum(value // bit for value in values), 2)
        return total

    turned = core * 4 + y
    mine = xor(turned, i, e)

    def label(m):
        return flip(mine, m ^ 6)

    def over(d):
        return flip(mine, (d % 2) * 4 + d // 2)

    def place(m):
        return (e * GROUP + flip(i, m), f)

    def side(d):
        return (p, flip(f, d))

    barrier = pltpu.get_barrier_semaphore()
    for q in range(EXPERTS):
        source = q * GROUP + mine

        @pl.when(source != p)
        def _():
            pl.semaphore_signal(barrier, inc=1, device_id=(source, f), device_id_type=MESH)

    for k in range(1, GROUP):
        pl.semaphore_signal(
            barrier, inc=1, device_id=(e * GROUP + turn(i + k, GROUP), f), device_id_type=MESH
        )
        pl.semaphore_signal(barrier, inc=1, device_id=(p, turn(f + k, FFN)), device_id_type=MESH)

    ids = ids_ref[...]
    onehot = iota((EXPERTS, TOK), 0) == ids
    earlier = jnp.where(iota((TOK, TOK), 0) < iota((TOK, TOK), 1), 1.0, 0.0).astype(BF16)
    before = jnp.dot(
        jnp.where(onehot, 1.0, 0.0).astype(BF16), earlier, preferred_element_type=F32
    )
    slot = jnp.sum(jnp.where(onehot, before, 0.0), axis=0, keepdims=True).astype(jnp.int32)
    pieces_row = iota((ROWS, PIECES * TOK), 0) - CAP * (iota((ROWS, PIECES * TOK), 1) // TOK)

    def build(expert, carry):
        place = jnp.where(ids == expert, slot, -ROWS * 2)
        place = jnp.concatenate([place] * PIECES, axis=1)
        select = jnp.where(pieces_row == place, 1.0, 0.0).astype(BF16)
        offset = xor(turned, expert, i) * BLK
        parts = []
        for ref in (tok_ref, cot_ref):
            for g in range(4):
                parts.append(ref[:, pl.ds(pl.multiple_of(offset + g * 128, 128), 128)])
        chunk_s[expert] = jnp.dot(
            select, jnp.concatenate(parts, axis=0), preferred_element_type=F32
        ).astype(BF16)
        return carry

    lax.fori_loop(0, EXPERTS, build, 0)

    pl.semaphore_wait(barrier, EXPERTS + 2 * (GROUP - 1) - jnp.where(mine == i, 1, 0))

    def routed(expert):
        target = expert * GROUP + xor(turned, expert, i)
        copy = pltpu.make_async_remote_copy(
            src_ref=chunk_s.at[expert], dst_ref=chunk_r.at[e],
            send_sem=a2a_ss.at[expert], recv_sem=a2a_rs.at[e],
            device_id=(target, f), device_id_type=MESH,
        )
        return target, copy

    for k in range(EXPERTS):
        target, copy = routed(turn(e + 4 + k, EXPERTS))

        @pl.when(target != p)
        def _():
            copy.start()

        @pl.when(target == p)
        def _():
            chunk_r[e] = chunk_s[e]

    def landed(q):
        return pltpu.make_async_remote_copy(
            src_ref=chunk_s.at[q], dst_ref=chunk_r.at[q],
            send_sem=a2a_ss.at[q], recv_sem=a2a_rs.at[q],
            device_id=(p, f), device_id_type=MESH,
        )

    for q in range(EXPERTS):
        @pl.when(q * GROUP + mine != p)
        def _():
            landed(q).wait_recv()

    received = chunk_r[...].reshape(EXPERTS * ROWS, 128)
    row_of = iota((ROWS, EXPERTS * ROWS), 0)
    source_of = lax.shift_right_logical(row_of * 3277, 16)
    gap = iota((ROWS, EXPERTS * ROWS), 1) - (ROWS - CAP) * source_of - row_of
    for piece in range(PIECES):
        select = jnp.where(gap == CAP * piece, 1.0, 0.0).astype(BF16)
        xall[mine, :, piece * 128 : (piece + 1) * 128] = jnp.dot(
            select, received, preferred_element_type=F32
        ).astype(BF16)

    def ring(chunk, start, size, device, index):
        rows = pl.ds(start, size)
        return pltpu.make_async_remote_copy(
            src_ref=xall.at[chunk, rows], dst_ref=xall.at[chunk, rows],
            send_sem=ring_ss.at[index], recv_sem=ring_rs.at[index],
            device_id=device, device_id_type=MESH,
        )

    half = ROWS // 2
    sent = []

    def go(copy):
        copy.start()
        sent.append(copy)

    def partial(m, target):
        x = label(m)
        target[:, :HID] = jnp.dot(xall[x, :, :BLK], win_ref[...], preferred_element_type=F32)
        target[:, HID:] = lax.dot_general(
            xall[x, :, BLK:], wout_ref[...], NT, preferred_element_type=F32
        )

    def relay(z, h):
        return pltpu.make_async_remote_copy(
            src_ref=part_s.at[2 + 4 * z, pl.ds(h * half, half)], dst_ref=relay_r.at[z, h],
            send_sem=rel_ss.at[2 * z + h], recv_sem=rel_rs.at[2 * z + h],
            device_id=place(1 + 2 * h), device_id_type=MESH,
        )

    def along_x(z, h):
        return pltpu.make_async_remote_copy(
            src_ref=part_s.at[4 * z + 3 - 2 * h], dst_ref=next_r.at[z, h],
            send_sem=nex_ss.at[2 * z + h], recv_sem=nex_rs.at[2 * z + h],
            device_id=place(3 - 2 * h), device_id_type=MESH,
        )

    def along_z():
        return pltpu.make_async_remote_copy(
            src_ref=part_s.at[4], dst_ref=pair_r,
            send_sem=par_ss.at[0], recv_sem=par_rs.at[0],
            device_id=place(4), device_id_type=MESH,
        )

    def far(z):
        partial(2 + 4 * z, work.at[z])
        part_s[2 + 4 * z] = work[z].astype(BF16)
        go(relay(z, 0))
        go(relay(z, 1))

    def near(z, h):
        m = 4 * z + 3 - 2 * h
        relay(z, h).wait_recv()
        if h:
            part_s[m, :half] = work[h, :half].astype(BF16)
            part_s[m, half:] = (work[h, half:] + relay_r[z, h].astype(F32)).astype(BF16)
        else:
            part_s[m, :half] = (work[h, :half] + relay_r[z, h].astype(F32)).astype(BF16)
            part_s[m, half:] = work[h, half:].astype(BF16)
        go(along_x(z, h))

    go(ring(mine, 0, ROWS, side(2), 0))
    go(ring(mine, 0, ROWS, side(6), 1))
    go(ring(mine, 0, ROWS, side(1), 2))
    far(1)
    ring(over(1), 0, ROWS, side(1), 2).wait_recv()
    far(0)
    ring(over(2), 0, ROWS, side(2), 0).wait_recv()
    go(ring(over(2), 0, half, side(6), 3))
    go(ring(over(2), 0, ROWS, side(1), 5))
    ring(over(6), 0, ROWS, side(6), 1).wait_recv()
    go(ring(over(6), half, half, side(2), 4))
    go(ring(over(6), 0, ROWS, side(1), 6))
    partial(7, work.at[0])
    partial(5, work.at[1])
    near(1, 0)
    near(1, 1)
    ring(over(3), 0, ROWS, side(1), 5).wait_recv()
    partial(3, work.at[0])
    ring(over(7), 0, ROWS, side(1), 6).wait_recv()
    partial(1, work.at[1])
    ring(over(4), 0, half, side(6), 3).wait_recv()
    go(ring(over(4), 0, half, side(1), 7))
    ring(over(4), half, half, side(2), 4).wait_recv()
    go(ring(over(4), half, half, side(1), 8))
    near(0, 0)
    near(0, 1)
    partial(4, acc.at[1])
    ring(over(5), 0, half, side(1), 7).wait_recv()
    ring(over(5), half, half, side(1), 8).wait_recv()
    partial(0, acc.at[0])
    for z in (1, 0):
        for h in (0, 1):
            along_x(z, h).wait_recv()
            acc[z] += next_r[z, h].astype(F32)
        if z:
            part_s[4] = acc[1].astype(BF16)
            go(along_z())
    along_z().wait_recv()

    owned = label(0)

    def activate(block, carry):
        rows = pl.ds(pl.multiple_of(block * 16, 16), 16)
        total = acc[0, rows, :] + pair_r[rows, :].astype(F32)
        act_value, act_slope = gelu_pair(total[:, :HID])
        hp[owned, rows, :HID] = act_value.astype(BF16)
        hp[owned, rows, HID:] = (total[:, HID:] * act_slope).astype(BF16)
        return carry

    lax.fori_loop(0, ROWS // 16, activate, 0)

    def spread(m, start, size, to, index):
        rows = pl.ds(start, size)
        return pltpu.make_async_remote_copy(
            src_ref=hp.at[label(m), rows], dst_ref=hp.at[label(m), rows],
            send_sem=ag_ss.at[index], recv_sem=ag_rs.at[index],
            device_id=place(to), device_id_type=MESH,
        )

    def grads(m, first=False):
        c = label(m)
        add_in = lax.dot_general(
            xall[c, :, :BLK], hp[c, :, HID:], TN, preferred_element_type=F32
        )
        add_out = lax.dot_general(
            hp[c, :, :HID], xall[c, :, BLK:], TN, preferred_element_type=F32
        )
        if first:
            gin[...] = add_in
            gout[...] = add_out
        else:
            gin[...] += add_in
            gout[...] += add_out

    go(spread(0, 0, ROWS, 4, 0))
    go(spread(0, 0, ROWS, 1, 1))
    go(spread(0, 0, ROWS, 3, 2))
    grads(0, True)
    spread(4, 0, ROWS, 4, 0).wait_recv()
    go(spread(4, 0, ROWS, 1, 3))
    go(spread(4, 0, ROWS, 3, 4))
    spread(1, 0, ROWS, 1, 1).wait_recv()
    go(spread(1, 0, half, 3, 5))
    spread(3, 0, ROWS, 3, 2).wait_recv()
    go(spread(3, half, half, 1, 6))
    grads(4)
    grads(1)
    grads(3)
    spread(2, 0, half, 3, 5).wait_recv()
    spread(2, half, half, 1, 6).wait_recv()
    spread(5, 0, ROWS, 1, 3).wait_recv()
    go(spread(5, 0, half, 3, 7))
    spread(7, 0, ROWS, 3, 4).wait_recv()
    go(spread(7, half, half, 1, 8))
    grads(2)
    grads(5)
    grads(7)
    spread(6, 0, half, 3, 7).wait_recv()
    spread(6, half, half, 1, 8).wait_recv()
    grads(6)

    def squares(ref, lanes, width, rows):
        def step(block, total):
            here = pl.ds(pl.multiple_of(block * 32, 32), 32)
            value = ref[here, :]
            value = value * value + EPS_ONE
            folded = value[:, :128]
            for g in range(1, width // 128):
                folded = folded + value[:, g * 128 : (g + 1) * 128]
            lanes[here, :] = folded
            return total + jnp.sum(value.reshape(4, 8, width), axis=0)

        total = lax.fori_loop(0, rows // 32, step, jnp.zeros((8, width), F32))
        return jnp.sum(total, axis=0, keepdims=True), jnp.sum(lanes[...].T, axis=0, keepdims=True)

    cols_in, rows_in = squares(gin, lane_in, HID, BLK)
    cols_out, rows_out = squares(gout, lane_out, BLK, HID)
    hidden_prev = hs_ref[:, pl.ds(e, 1), :]
    width_prev = ws_ref[:, pl.ds(e, 1), pl.ds(pl.multiple_of(i * BLK, BLK), BLK)]
    hidden_sum = jnp.sum(hidden_prev[1], axis=1, keepdims=True)
    stat_h[i] = jnp.concatenate([cols_in, rows_out, jnp.zeros((6, HID), F32)], axis=0)
    stat_w[f] = jnp.concatenate(
        [rows_in, cols_out, jnp.broadcast_to(hidden_sum, (6, BLK))], axis=0
    )

    def exchange(buf, own, ssem, rsem, device):
        copies = []
        for k in range(1, 8):
            d = turn(own + k, 8)
            copies.append((
                pltpu.make_async_remote_copy(
                    src_ref=buf.at[own], dst_ref=buf.at[own],
                    send_sem=ssem.at[d], recv_sem=rsem.at[own],
                    device_id=device(d), device_id_type=MESH,
                ),
                pltpu.make_async_remote_copy(
                    src_ref=buf.at[d], dst_ref=buf.at[d],
                    send_sem=ssem.at[d], recv_sem=rsem.at[d],
                    device_id=device(d), device_id_type=MESH,
                ),
            ))
        return copies

    def in_group(d):
        return (e * GROUP + d, f)

    def in_ffn(d):
        return (p, d)

    over_group = exchange(stat_h, i, sh_ss, sh_rs, in_group)
    over_ffn = exchange(stat_w, f, sw_ss, sw_rs, in_ffn)
    for start, _ in over_group + over_ffn:
        start.start()
    for _, arrival in over_group + over_ffn:
        arrival.wait_recv()
    sum_h = jnp.sum(stat_h[...], axis=0)
    sum_w = jnp.sum(stat_w[...], axis=0)

    cols_in = DECAY_RATE * hidden_prev[0] + (1.0 - DECAY_RATE) * sum_h[0:1] / D
    rows_out = DECAY_RATE * hidden_prev[1] + (1.0 - DECAY_RATE) * sum_h[1:2] / D
    rows_in = DECAY_RATE * width_prev[0] + (1.0 - DECAY_RATE) * sum_w[0:1] / FF
    cols_out = DECAY_RATE * width_prev[1] + (1.0 - DECAY_RATE) * sum_w[1:2] / FF
    lane_in[...] = jnp.broadcast_to(lax.rsqrt(rows_in), (128, BLK)).T
    lane_out[...] = jnp.broadcast_to(lax.rsqrt(rows_out), (128, HID)).T
    scale_in = lax.rsqrt(cols_in)
    scale_out = lax.rsqrt(cols_out)

    def scaled(ref, lanes, scale, width, rows):
        def step(block, total):
            here = pl.ds(pl.multiple_of(block * 32, 32), 32)
            factor = lanes[here, :]
            for g in range(width // 128):
                cols = slice(g * 128, (g + 1) * 128)
                value = ref[here, cols] * factor * scale[:, cols]
                ref[here, cols] = value
                total = total + jnp.sum((value * value).reshape(4, 8, 128), axis=0)
            return total

        total = lax.fori_loop(0, rows // 32, step, jnp.zeros((8, 128), F32))
        return jnp.sum(total, axis=0, keepdims=True)

    norm_in = scaled(gin, lane_in, scale_in, HID, BLK)
    norm_out = scaled(gout, lane_out, scale_out, BLK, HID)

    def fold(row):
        total = row[:, :128]
        for g in range(1, row.shape[1] // 128):
            total = total + row[:, g * 128 : (g + 1) * 128]
        return total

    norm_g[i] = jnp.concatenate(
        [norm_in, norm_out, fold(sum_w[0:1]), fold(sum_w[1:2]), jnp.zeros((4, 128), F32)], axis=0
    )
    group_norms = exchange(norm_g, i, ng_ss, ng_rs, in_group)
    for start, _ in group_norms:
        start.start()
    for _, arrival in group_norms:
        arrival.wait_recv()
    group_sum = jnp.sum(norm_g[...], axis=0)
    norm_f[f] = group_sum
    ffn_norms = exchange(norm_f, f, nf_ss, nf_rs, in_ffn)
    for start, _ in ffn_norms:
        start.start()
    for _, arrival in ffn_norms:
        arrival.wait_recv()
    norm_sum = jnp.sum(jnp.sum(norm_f[...], axis=0), axis=1, keepdims=True)
    totals = jnp.sum(group_sum, axis=1, keepdims=True)

    whole_count = float(D) * float(FF)
    width_mean = jnp.sum(ws_ref[0, pl.ds(e, 1), :], axis=1, keepdims=True) / D
    mean_in = DECAY_RATE * width_mean + (1.0 - DECAY_RATE) * totals[2:3] / whole_count
    mean_out = (
        DECAY_RATE * sum_w[2:3, 0:1] / FF + (1.0 - DECAY_RATE) * totals[3:4] / whole_count
    )
    def last_factor(mean, norm):
        return jnp.sqrt(mean) / jnp.maximum(1.0, jnp.sqrt(mean * (norm / whole_count)))

    factor_in = last_factor(mean_in, norm_sum[0:1])
    factor_out = last_factor(mean_out, norm_sum[1:2])

    def store_in(block, carry):
        here = pl.ds(pl.multiple_of(block * 32, 32), 32)
        uin_ref[here, :] = (gin[here, :] * factor_in).astype(BF16)
        return carry

    def store_out(block, carry):
        here = pl.ds(pl.multiple_of(block * 32, 32), 32)
        uout_ref[here, :] = (gout[here, :] * factor_out).astype(BF16)
        return carry

    lax.fori_loop(0, BLK // 32, store_in, 0)
    lax.fori_loop(0, HID // 32, store_out, 0)

    for q in range(EXPERTS):
        target, copy = routed(q)

        @pl.when(target != p)
        def _():
            copy.wait_send()

    for copy in sent:
        copy.wait_send()
    for start, _ in over_group + over_ffn + group_norms + ffn_norms:
        start.wait_send()


def shards(tokens, cotangent, expert_ids, in_weight, out_weight, width_states, hidden_states):
    vmem = pl.BlockSpec(memory_space=pltpu.VMEM)
    def dma(count):
        return pltpu.SemaphoreType.DMA((count,))

    dma8 = dma(8)
    update_in, update_out = pl.pallas_call(
        kernel,
        out_shape=(
            jax.ShapeDtypeStruct((BLK, HID), BF16),
            jax.ShapeDtypeStruct((HID, BLK), BF16),
        ),
        in_specs=[vmem] * 7,
        out_specs=(vmem, vmem),
        scratch_shapes=[
            pltpu.VMEM((EXPERTS, ROWS, 128), BF16),
            pltpu.VMEM((EXPERTS, ROWS, 128), BF16),
            pltpu.VMEM((GROUP, ROWS, 2 * BLK), BF16),
            pltpu.VMEM((GROUP, ROWS, 2 * HID), BF16),
            pltpu.VMEM((2, 2, ROWS // 2, 2 * HID), BF16),
            pltpu.VMEM((2, 2, ROWS, 2 * HID), BF16),
            pltpu.VMEM((ROWS, 2 * HID), BF16),
            pltpu.VMEM((2, ROWS, 2 * HID), F32),
            pltpu.VMEM((2, ROWS, 2 * HID), F32),
            pltpu.VMEM((GROUP, ROWS, 2 * HID), BF16),
            pltpu.VMEM((BLK, HID), F32),
            pltpu.VMEM((HID, BLK), F32),
            pltpu.VMEM((BLK, 128), F32),
            pltpu.VMEM((HID, 128), F32),
            pltpu.VMEM((GROUP, 8, HID), F32),
            pltpu.VMEM((FFN, 8, BLK), F32),
            pltpu.VMEM((GROUP, 8, 128), F32),
            pltpu.VMEM((FFN, 8, 128), F32),
            dma8, dma8, dma(9), dma(9), dma(4), dma(4), dma(4), dma(4), dma(1), dma(1),
            dma(9), dma(9), dma8, dma8, dma8, dma8, dma8, dma8, dma8, dma8,
        ],
        compiler_params=pltpu.CompilerParams(
            collective_id=0, has_side_effects=True, vmem_limit_bytes=56 * 1024 * 1024
        ),
        name="switch_update",
    )(
        expert_ids.reshape(1, TOK), tokens, cotangent, in_weight[0], out_weight[0],
        width_states, hidden_states,
    )
    return (update_in[None], update_out[None])


def solution(mesh):
    return jax.shard_map(
        shards,
        mesh=mesh,
        in_specs=(
            P("expert", None),
            P("expert", None),
            P("expert", None),
            P("expert", None, "ffn"),
            P("expert", "ffn", None),
            P(),
            P(None, None, "ffn"),
        ),
        out_specs=(P("expert", None, "ffn"), P("expert", "ffn", None)),
        check_vma=False,
    )
```

```python
import math

import jax
import jax.numpy as jnp
from jax import lax
from jax.experimental import pallas as pl
from jax.experimental.pallas import tpu as pltpu
from jax.sharding import PartitionSpec as P

D = 4096
FF = 5120
GROUP = 8
EXPERTS = 8
FFN = 8
CAP = 20
BLK = D // GROUP
HID = FF // FFN
TOK = 128
ROWS = GROUP * CAP
PIECES = BLK // 128
SEND = PIECES * CAP

DECAY_RATE = 0.9
EPS_ONE = 1e-30
ROOT_COEF = math.sqrt(2.0 / math.pi)
CUBIC_COEF = 0.044715

MESH = pl.DeviceIdType.MESH
F32 = jnp.float32
BF16 = jnp.bfloat16
NT = (((1,), (1,)), ((), ()))
TN = (((0,), (0,)), ((), ()))


def gelu_pair(inputs):
    inner = ROOT_COEF * (inputs + CUBIC_COEF * inputs * inputs * inputs)
    tangent = jnp.tanh(inner)
    act_value = 0.5 * inputs * (1.0 + tangent)
    act_slope = 0.5 * (1.0 + tangent) + 0.5 * inputs * (1.0 - tangent * tangent) * ROOT_COEF * (
        1.0 + 3.0 * CUBIC_COEF * inputs * inputs
    )
    return (act_value, act_slope)


def iota(shape, dim):
    return lax.broadcasted_iota(jnp.int32, shape, dim)


def kernel(
    ids_any, tok_any, cot_any, win_any, wout_any, ws_any, hs_any,
    raw_in, raw_out, factor_in, factor_out,
    ids_ref, tok_ref, cot_ref, win_ref, wout_ref, ws_ref, hs_ref,
    chunk_s, chunk_r, xall, part_s, relay_r, next_r, pair_r, far_r, work, acc, slope, hp, gin, gout,
    lane_in, lane_out, stat_h, stat_w, norm_g, norm_f,
    a2a_ss, a2a_rs, ring_ss, ring_rs, rel_ss, rel_rs, nex_ss, nex_rs, par_ss, par_rs, far_ss, far_rs, ag_ss, ag_rs,
    sh_ss, sh_rs, sw_ss, sw_rs, ng_ss, ng_rs, nf_ss, nf_rs,
    load_sem, save_sem,
):
    p = lax.axis_index("expert")
    f = lax.axis_index("ffn")
    e = p // GROUP
    i = p % GROUP
    y = f // 2
    core = f % 2

    def turn(value, n):
        return lax.rem(value, n)

    def flip(value, mask):
        for bit in (1, 2, 4):
            if mask & bit:
                value = value + bit * (1 - 2 * turn(value // bit, 2))
        return value

    def xor(*values):
        total = 0
        for bit in (1, 2, 4):
            total = total + bit * turn(sum(value // bit for value in values), 2)
        return total

    turned = core * 4 + y
    mine = xor(turned, i, e)

    def label(m):
        return flip(mine, m ^ 6)

    def over(d):
        return flip(mine, (d % 2) * 4 + d // 2)

    def place(m):
        return (e * GROUP + flip(i, m), f)

    def side(d):
        return (p, flip(f, d))

    loads = [
        pltpu.make_async_copy(source, here, load_sem.at[index])
        for index, (source, here) in enumerate((
            (ids_any, ids_ref), (tok_any, tok_ref), (cot_any, cot_ref), (win_any, win_ref),
            (wout_any, wout_ref), (ws_any, ws_ref), (hs_any, hs_ref),
        ))
    ]
    for load in loads:
        load.start()

    barrier = pltpu.get_barrier_semaphore()
    for q in range(EXPERTS):
        source = q * GROUP + mine

        @pl.when(source != p)
        def _():
            pl.semaphore_signal(barrier, inc=1, device_id=(source, f), device_id_type=MESH)

    for k in range(1, GROUP):
        pl.semaphore_signal(
            barrier, inc=1, device_id=(e * GROUP + turn(i + k, GROUP), f), device_id_type=MESH
        )
        pl.semaphore_signal(barrier, inc=1, device_id=(p, turn(f + k, FFN)), device_id_type=MESH)

    loads[0].wait()
    ids = ids_ref[...]
    onehot = iota((EXPERTS, TOK), 0) == ids
    earlier = jnp.where(iota((TOK, TOK), 0) < iota((TOK, TOK), 1), 1.0, 0.0).astype(BF16)
    before = jnp.dot(
        jnp.where(onehot, 1.0, 0.0).astype(BF16), earlier, preferred_element_type=F32
    )
    slot = jnp.sum(jnp.where(onehot, before, 0.0), axis=0, keepdims=True).astype(jnp.int32)
    pieces_row = iota((SEND, PIECES * TOK), 0) - CAP * (iota((SEND, PIECES * TOK), 1) // TOK)

    def build(a, ref):
        def step(expert, carry):
            place = jnp.where(ids == expert, slot, -ROWS * 2)
            place = jnp.concatenate([place] * PIECES, axis=1)
            select = jnp.where(pieces_row == place, 1.0, 0.0).astype(BF16)
            offset = xor(turned, expert, i) * BLK
            parts = [
                ref[:, pl.ds(pl.multiple_of(offset + g * 128, 128), 128)] for g in range(PIECES)
            ]
            chunk_s[a, expert] = jnp.dot(
                select, jnp.concatenate(parts, axis=0), preferred_element_type=F32
            ).astype(BF16)
            return carry

        loads[1 + a].wait()
        lax.fori_loop(0, EXPERTS, step, 0)

    build(0, tok_ref)
    pl.semaphore_wait(barrier, EXPERTS + 2 * (GROUP - 1) - jnp.where(mine == i, 1, 0))

    def routed(a, expert):
        target = expert * GROUP + xor(turned, expert, i)
        copy = pltpu.make_async_remote_copy(
            src_ref=chunk_s.at[a, expert], dst_ref=chunk_r.at[a, e],
            send_sem=a2a_ss.at[a, expert], recv_sem=a2a_rs.at[a, e],
            device_id=(target, f), device_id_type=MESH,
        )
        return target, copy

    def route(a):
        for k in range(EXPERTS):
            target, copy = routed(a, turn(e + 4 + k, EXPERTS))

            @pl.when(target != p)
            def _():
                copy.start()

            @pl.when(target == p)
            def _():
                chunk_r[a, e] = chunk_s[a, e]

    def arrived(a):
        for q in range(EXPERTS):
            @pl.when(q * GROUP + mine != p)
            def _():
                pltpu.make_async_remote_copy(
                    src_ref=chunk_s.at[a, q], dst_ref=chunk_r.at[a, q],
                    send_sem=a2a_ss.at[a, q], recv_sem=a2a_rs.at[a, q],
                    device_id=(p, f), device_id_type=MESH,
                ).wait_recv()

    def unpack(a):
        received = chunk_r[a].reshape(EXPERTS * SEND, 128)
        row_of = iota((ROWS, EXPERTS * SEND), 0)
        source_of = lax.shift_right_logical(row_of * 3277, 16)
        gap = iota((ROWS, EXPERTS * SEND), 1) - (SEND - CAP) * source_of - row_of
        for piece in range(PIECES):
            select = jnp.where(gap == CAP * piece, 1.0, 0.0).astype(BF16)
            xall[a, mine, :, piece * 128 : (piece + 1) * 128] = jnp.dot(
                select, received, preferred_element_type=F32
            ).astype(BF16)

    def ring(a, chunk, start, size, device, index):
        rows = pl.ds(start, size)
        return pltpu.make_async_remote_copy(
            src_ref=xall.at[a, chunk, rows], dst_ref=xall.at[a, chunk, rows],
            send_sem=ring_ss.at[a, index], recv_sem=ring_rs.at[a, index],
            device_id=device, device_id_type=MESH,
        )

    half = ROWS // 2
    sent = []

    def go(copy):
        copy.start()
        sent.append(copy)

    def partial(a, m):
        x = xall[a, label(m)]
        if a:
            return lax.dot_general(x, wout_ref[...], NT, preferred_element_type=F32)
        return jnp.dot(x, win_ref[...], preferred_element_type=F32)

    def relay(a, z, h):
        return pltpu.make_async_remote_copy(
            src_ref=part_s.at[a, 2 + 4 * z, pl.ds(h * half, half)], dst_ref=relay_r.at[a, z, h],
            send_sem=rel_ss.at[a, 2 * z + h], recv_sem=rel_rs.at[a, 2 * z + h],
            device_id=place(1 + 2 * h), device_id_type=MESH,
        )

    def along_x(a, z, h):
        return pltpu.make_async_remote_copy(
            src_ref=part_s.at[a, 4 * z + 3 - 2 * h], dst_ref=next_r.at[a, z, h],
            send_sem=nex_ss.at[a, 2 * z + h], recv_sem=nex_rs.at[a, 2 * z + h],
            device_id=place(3 - 2 * h), device_id_type=MESH,
        )

    def along_z(a):
        return pltpu.make_async_remote_copy(
            src_ref=part_s.at[a, 4], dst_ref=pair_r.at[a],
            send_sem=par_ss.at[a], recv_sem=par_rs.at[a],
            device_id=place(4), device_id_type=MESH,
        )

    def far_z():
        return pltpu.make_async_remote_copy(
            src_ref=part_s.at[1, 6], dst_ref=far_r,
            send_sem=far_ss.at[0], recv_sem=far_rs.at[0],
            device_id=place(4), device_id_type=MESH,
        )

    def far(a, z):
        part_s[a, 2 + 4 * z] = partial(a, 2 + 4 * z).astype(BF16)
        go(relay(a, z, 0))
        go(relay(a, z, 1))

    def near(a, z):
        for h in (0, 1):
            work[h] = partial(a, 4 * z + 3 - 2 * h)
        for h in (0, 1):
            m = 4 * z + 3 - 2 * h
            if a and z:
                part_s[a, m] = work[h].astype(BF16)
                go(along_x(a, z, h))
                continue
            relay(a, z, h).wait_recv()
            met, other = pl.ds(h * half, half), pl.ds((1 - h) * half, half)
            part_s[a, m, other] = work[h, other].astype(BF16)
            part_s[a, m, met] = (work[h, met] + relay_r[a, z, h].astype(F32)).astype(BF16)
            go(along_x(a, z, h))

    def ring_open(a):
        go(ring(a, mine, 0, ROWS, side(2), 0))
        go(ring(a, mine, 0, ROWS, side(6), 1))
        go(ring(a, mine, 0, ROWS, side(1), 2))

    def ring_pass(a):
        ring(a, over(2), 0, ROWS, side(2), 0).wait_recv()
        go(ring(a, over(2), 0, half, side(6), 3))
        go(ring(a, over(2), 0, ROWS, side(1), 5))
        ring(a, over(6), 0, ROWS, side(6), 1).wait_recv()
        go(ring(a, over(6), half, half, side(2), 4))
        go(ring(a, over(6), 0, ROWS, side(1), 6))

    def ring_halves(a):
        ring(a, over(4), 0, half, side(6), 3).wait_recv()
        go(ring(a, over(4), 0, half, side(1), 7))
        ring(a, over(4), half, half, side(2), 4).wait_recv()
        go(ring(a, over(4), half, half, side(1), 8))

    def far_pair(a):
        ring(a, over(1), 0, ROWS, side(1), 2).wait_recv()
        far(a, 0)

    def near_pair(a):
        ring(a, over(3), 0, ROWS, side(1), 5).wait_recv()
        ring(a, over(7), 0, ROWS, side(1), 6).wait_recv()
        near(a, 0)

    def own_column(a):
        acc[a, 1] = partial(a, 4)
        ring(a, over(5), 0, half, side(1), 7).wait_recv()
        ring(a, over(5), half, half, side(1), 8).wait_recv()
        acc[a, 0] = partial(a, 0)

    def sum_x(a, z):
        along_x(a, z, 0).wait_recv()
        along_x(a, z, 1).wait_recv()
        total = acc[a, z] + next_r[a, z, 0].astype(F32) + next_r[a, z, 1].astype(F32)
        if z:
            part_s[a, 4] = total.astype(BF16)
            go(along_z(a))
        else:
            acc[a, 0] = total

    route(0)
    build(1, cot_ref)
    arrived(0)
    route(1)
    unpack(0)
    ring_open(0)
    for load in loads[3:]:
        load.wait()
    far(0, 1)
    far_pair(0)
    ring_pass(0)
    near(0, 1)
    near_pair(0)
    ring_halves(0)
    arrived(1)
    unpack(1)
    ring_open(1)
    part_s[1, 6] = partial(1, 6).astype(BF16)
    go(far_z())
    own_column(0)
    sum_x(0, 1)
    ring(1, over(1), 0, ROWS, side(1), 2).wait_recv()
    work[0] = partial(1, 2)
    ring_pass(1)
    far_z().wait_recv()
    part_s[1, 2] = (work[0] + far_r[...].astype(F32)).astype(BF16)
    go(relay(1, 0, 0))
    go(relay(1, 0, 1))
    near(1, 1)
    ring_halves(1)
    sum_x(0, 0)
    along_z(0).wait_recv()

    owned = label(0)

    def activate(block, carry):
        rows = pl.ds(pl.multiple_of(block * 16, 16), 16)
        act_value, act_slope = gelu_pair(acc[0, 0, rows, :] + pair_r[0, rows, :].astype(F32))
        hp[0, owned, rows, :] = act_value.astype(BF16)
        slope[rows, :] = act_slope
        return carry

    def backward(block, carry):
        rows = pl.ds(pl.multiple_of(block * 16, 16), 16)
        back = acc[1, 0, rows, :] + pair_r[1, rows, :].astype(F32)
        hp[1, owned, rows, :] = (back * slope[rows, :]).astype(BF16)
        return carry

    def spread(a, m, start, size, to, index):
        rows = pl.ds(start, size)
        return pltpu.make_async_remote_copy(
            src_ref=hp.at[a, label(m), rows], dst_ref=hp.at[a, label(m), rows],
            send_sem=ag_ss.at[a, index], recv_sem=ag_rs.at[a, index],
            device_id=place(to), device_id_type=MESH,
        )

    def open_spread(a):
        go(spread(a, 0, 0, ROWS, 4, 0))
        go(spread(a, 0, 0, ROWS, 1, 1))
        go(spread(a, 0, 0, ROWS, 3, 2))

    def pass_pair(a):
        spread(a, 4, 0, ROWS, 4, 0).wait_recv()
        go(spread(a, 4, 0, ROWS, 1, 3))
        go(spread(a, 4, 0, ROWS, 3, 4))

    def pass_next(a):
        spread(a, 1, 0, ROWS, 1, 1).wait_recv()
        go(spread(a, 1, 0, half, 3, 5))
        spread(a, 3, 0, ROWS, 3, 2).wait_recv()
        go(spread(a, 3, half, half, 1, 6))

    def wait_far(a):
        spread(a, 2, 0, half, 3, 5).wait_recv()
        spread(a, 2, half, half, 1, 6).wait_recv()

    def pass_pair_next(a):
        spread(a, 5, 0, ROWS, 1, 3).wait_recv()
        go(spread(a, 5, 0, half, 3, 7))
        spread(a, 7, 0, ROWS, 3, 4).wait_recv()
        go(spread(a, 7, half, half, 1, 8))

    def wait_pair_far(a):
        spread(a, 6, 0, half, 3, 7).wait_recv()
        spread(a, 6, half, half, 1, 8).wait_recv()

    def grads(a, m, first=False):
        c = label(m)
        if a:
            add, total = lax.dot_general(
                xall[0, c], hp[1, c], TN, preferred_element_type=F32
            ), gin
        else:
            add, total = lax.dot_general(
                hp[0, c], xall[1, c], TN, preferred_element_type=F32
            ), gout
        if first:
            total[...] = add
        else:
            total[...] += add

    lax.fori_loop(0, ROWS // 16, activate, 0)
    open_spread(0)
    near_pair(1)
    own_column(1)
    sum_x(1, 1)
    pass_pair(0)
    sum_x(1, 0)
    along_z(1).wait_recv()
    lax.fori_loop(0, ROWS // 16, backward, 0)
    open_spread(1)
    grads(0, 0, True)
    grads(0, 4)
    pass_next(0)
    pass_pair(1)
    grads(0, 1)
    grads(0, 3)
    wait_far(0)
    go(spread(0, 2, 0, ROWS, 4, 7))
    grads(0, 2)
    pass_next(1)
    spread(0, 5, 0, ROWS, 1, 3).wait_recv()
    grads(0, 5)
    spread(0, 7, 0, ROWS, 3, 4).wait_recv()
    grads(0, 7)
    grads(1, 0, True)
    grads(1, 4)
    grads(1, 1)
    grads(1, 3)
    pass_pair_next(1)
    grads(1, 5)
    grads(1, 7)
    spread(0, 6, 0, ROWS, 4, 7).wait_recv()
    grads(0, 6)
    wait_far(1)
    grads(1, 2)

    def squares(ref, lanes, width, rows):
        def step(block, total):
            here = pl.ds(pl.multiple_of(block * 32, 32), 32)
            value = ref[here, :]
            value = value * value + EPS_ONE
            folded = value[:, :128]
            for g in range(1, width // 128):
                folded = folded + value[:, g * 128 : (g + 1) * 128]
            lanes[here, :] = folded
            return total + jnp.sum(value.reshape(4, 8, width), axis=0)

        total = lax.fori_loop(0, rows // 32, step, jnp.zeros((8, width), F32))
        return jnp.sum(total, axis=0, keepdims=True), jnp.sum(lanes[...].T, axis=0, keepdims=True)

    hidden_prev = hs_ref[:, pl.ds(e, 1), :]
    width_prev = ws_ref[:, pl.ds(e, 1), pl.ds(pl.multiple_of(i * BLK, BLK), BLK)]

    def exchange(at, own, ssem, rsem, device):
        copies = []
        for k in range(1, 8):
            d = turn(own + k, 8)
            copies.append((
                pltpu.make_async_remote_copy(
                    src_ref=at(own), dst_ref=at(own),
                    send_sem=ssem(d), recv_sem=rsem(own),
                    device_id=device(d), device_id_type=MESH,
                ),
                pltpu.make_async_remote_copy(
                    src_ref=at(d), dst_ref=at(d),
                    send_sem=ssem(d), recv_sem=rsem(d),
                    device_id=device(d), device_id_type=MESH,
                ),
            ))
        return copies

    def in_group(d):
        return (e * GROUP + d, f)

    def in_ffn(d):
        return (p, d)

    def both(a):
        return exchange(
            lambda d: stat_h.at[a, d], i, lambda d: sh_ss.at[a, d], lambda d: sh_rs.at[a, d],
            in_group,
        ) + exchange(
            lambda d: stat_w.at[a, d], f, lambda d: sw_ss.at[a, d], lambda d: sw_rs.at[a, d],
            in_ffn,
        )

    stats = [both(0), both(1)]

    cols_out, rows_out = squares(gout, lane_out, BLK, HID)
    hidden_sum = jnp.sum(hidden_prev[1], axis=1, keepdims=True)
    stat_h[0, i] = jnp.broadcast_to(rows_out, (8, HID))
    stat_w[0, f] = jnp.concatenate([cols_out, jnp.broadcast_to(hidden_sum, (7, BLK))], axis=0)
    for start, _ in stats[0]:
        start.start()

    wait_pair_far(1)
    grads(1, 6)
    cols_in, rows_in = squares(gin, lane_in, HID, BLK)
    stat_h[1, i] = jnp.broadcast_to(cols_in, (8, HID))
    stat_w[1, f] = jnp.broadcast_to(rows_in, (8, BLK))
    for start, _ in stats[1]:
        start.start()

    def scaled(ref, lanes, scale, width, rows):
        def step(block, total):
            here = pl.ds(pl.multiple_of(block * 32, 32), 32)
            factor = lanes[here, :]
            for g in range(width // 128):
                cols = slice(g * 128, (g + 1) * 128)
                value = ref[here, cols] * factor * scale[:, cols]
                ref[here, cols] = value
                total = total + jnp.sum((value * value).reshape(4, 8, 128), axis=0)
            return total

        total = lax.fori_loop(0, rows // 32, step, jnp.zeros((8, 128), F32))
        return jnp.sum(total, axis=0, keepdims=True)

    for _, arrival in stats[0]:
        arrival.wait_recv()
    sum_out = jnp.sum(stat_w[0], axis=0)
    rows_out = DECAY_RATE * hidden_prev[1] + (1.0 - DECAY_RATE) * (
        jnp.sum(stat_h[0], axis=0)[0:1] / D
    )
    cols_out = DECAY_RATE * width_prev[1] + (1.0 - DECAY_RATE) * sum_out[0:1] / FF
    lane_out[...] = jnp.broadcast_to(lax.rsqrt(rows_out), (128, HID)).T
    norm_out = scaled(gout, lane_out, lax.rsqrt(cols_out), BLK, HID)
    save_out = pltpu.make_async_copy(gout, raw_out, save_sem.at[0])
    save_out.start()

    for _, arrival in stats[1]:
        arrival.wait_recv()
    sum_in = jnp.sum(stat_w[1], axis=0)
    cols_in = DECAY_RATE * hidden_prev[0] + (1.0 - DECAY_RATE) * (
        jnp.sum(stat_h[1], axis=0)[0:1] / D
    )
    rows_in = DECAY_RATE * width_prev[0] + (1.0 - DECAY_RATE) * sum_in[0:1] / FF
    lane_in[...] = jnp.broadcast_to(lax.rsqrt(rows_in), (128, BLK)).T
    norm_in = scaled(gin, lane_in, lax.rsqrt(cols_in), HID, BLK)
    save_in = pltpu.make_async_copy(gin, raw_in, save_sem.at[1])
    save_in.start()

    def fold(row):
        total = row[:, :128]
        for g in range(1, row.shape[1] // 128):
            total = total + row[:, g * 128 : (g + 1) * 128]
        return total

    norm_g[i] = jnp.concatenate(
        [norm_in, norm_out, fold(sum_in[0:1]), fold(sum_out[0:1]), jnp.zeros((4, 128), F32)], axis=0
    )
    group_norms = exchange(
        lambda d: norm_g.at[d], i, lambda d: ng_ss.at[d], lambda d: ng_rs.at[d], in_group
    )
    for start, _ in group_norms:
        start.start()
    for _, arrival in group_norms:
        arrival.wait_recv()
    group_sum = jnp.sum(norm_g[...], axis=0)
    norm_f[f] = group_sum
    ffn_norms = exchange(
        lambda d: norm_f.at[d], f, lambda d: nf_ss.at[d], lambda d: nf_rs.at[d], in_ffn
    )
    for start, _ in ffn_norms:
        start.start()
    for _, arrival in ffn_norms:
        arrival.wait_recv()
    norm_sum = jnp.sum(jnp.sum(norm_f[...], axis=0), axis=1, keepdims=True)
    totals = jnp.sum(group_sum, axis=1, keepdims=True)

    whole_count = float(D) * float(FF)
    width_mean = jnp.sum(ws_ref[0, pl.ds(e, 1), :], axis=1, keepdims=True) / D
    mean_in = DECAY_RATE * width_mean + (1.0 - DECAY_RATE) * totals[2:3] / whole_count
    mean_out = (
        DECAY_RATE * sum_out[1:2, 0:1] / FF + (1.0 - DECAY_RATE) * totals[3:4] / whole_count
    )
    def last_factor(mean, norm):
        return jnp.sqrt(mean) / jnp.maximum(1.0, jnp.sqrt(mean * (norm / whole_count)))

    factor_in[...] = last_factor(mean_in, norm_sum[0:1])
    factor_out[...] = last_factor(mean_out, norm_sum[1:2])

    save_in.wait()
    save_out.wait()
    for a in range(2):
        for q in range(EXPERTS):
            target, copy = routed(a, q)

            @pl.when(target != p)
            def _():
                copy.wait_send()

    for copy in sent:
        copy.wait_send()
    for start, _ in stats[0] + stats[1] + group_norms + ffn_norms:
        start.wait_send()


def shards(tokens, cotangent, expert_ids, in_weight, out_weight, width_states, hidden_states):
    vmem = pl.BlockSpec(memory_space=pltpu.VMEM)
    anywhere = pl.BlockSpec(memory_space=pl.ANY)

    def dma(*shape):
        return pltpu.SemaphoreType.DMA(shape)

    operands = (
        expert_ids.reshape(1, TOK), tokens, cotangent, in_weight[0], out_weight[0],
        width_states, hidden_states,
    )
    raw_in, raw_out, factor_in, factor_out = pl.pallas_call(
        kernel,
        out_shape=(
            jax.ShapeDtypeStruct((BLK, HID), F32),
            jax.ShapeDtypeStruct((HID, BLK), F32),
            jax.ShapeDtypeStruct((1, 1), F32),
            jax.ShapeDtypeStruct((1, 1), F32),
        ),
        in_specs=[anywhere] * 7,
        out_specs=(anywhere, anywhere, vmem, vmem),
        scratch_shapes=[pltpu.VMEM(value.shape, value.dtype) for value in operands]
        + [
            pltpu.VMEM((2, EXPERTS, SEND, 128), BF16),
            pltpu.VMEM((2, EXPERTS, SEND, 128), BF16),
            pltpu.VMEM((2, GROUP, ROWS, BLK), BF16),
            pltpu.VMEM((2, GROUP, ROWS, HID), BF16),
            pltpu.VMEM((2, 2, 2, ROWS // 2, HID), BF16),
            pltpu.VMEM((2, 2, 2, ROWS, HID), BF16),
            pltpu.VMEM((2, ROWS, HID), BF16),
            pltpu.VMEM((ROWS, HID), BF16),
            pltpu.VMEM((2, ROWS, HID), F32),
            pltpu.VMEM((2, 2, ROWS, HID), F32),
            pltpu.VMEM((ROWS, HID), F32),
            pltpu.VMEM((2, GROUP, ROWS, HID), BF16),
            pltpu.VMEM((BLK, HID), F32),
            pltpu.VMEM((HID, BLK), F32),
            pltpu.VMEM((BLK, 128), F32),
            pltpu.VMEM((HID, 128), F32),
            pltpu.VMEM((2, GROUP, 8, HID), F32),
            pltpu.VMEM((2, FFN, 8, BLK), F32),
            pltpu.VMEM((GROUP, 8, 128), F32),
            pltpu.VMEM((FFN, 8, 128), F32),
            dma(2, 8), dma(2, 8), dma(2, 9), dma(2, 9), dma(2, 4), dma(2, 4), dma(2, 4),
            dma(2, 4), dma(2), dma(2), dma(1), dma(1), dma(2, 9), dma(2, 9),
            dma(2, 8), dma(2, 8), dma(2, 8), dma(2, 8), dma(8), dma(8), dma(8), dma(8),
            dma(7), dma(2),
        ],
        compiler_params=pltpu.CompilerParams(
            collective_id=0, has_side_effects=True, vmem_limit_bytes=56 * 1024 * 1024
        ),
        name="switch_update",
    )(*operands)
    update_in = (raw_in * factor_in).astype(BF16)
    update_out = (raw_out * factor_out).astype(BF16)
    return (update_in[None], update_out[None])


def solution(mesh):
    return jax.shard_map(
        shards,
        mesh=mesh,
        in_specs=(
            P("expert", None),
            P("expert", None),
            P("expert", None),
            P("expert", None, "ffn"),
            P("expert", "ffn", None),
            P(),
            P(None, None, "ffn"),
        ),
        out_specs=(P("expert", None, "ffn"), P("expert", "ffn", None)),
        check_vma=False,
    )
```

```python
import math

import jax
import jax.numpy as jnp
from jax import lax
from jax.experimental import pallas as pl
from jax.experimental.pallas import tpu as pltpu
from jax.sharding import PartitionSpec as P

D = 4096
FF = 5120
GROUP = 8
EXPERTS = 8
FFN = 8
CAP = 20
BLK = D // GROUP
HID = FF // FFN
TOK = 128
ROWS = GROUP * CAP
PIECES = BLK // 128
SEND = PIECES * CAP
SPLIT = 4

DECAY_RATE = 0.9
EPS_ONE = 1e-30
ROOT_COEF = math.sqrt(2.0 / math.pi)
CUBIC_COEF = 0.044715

MESH = pl.DeviceIdType.MESH
F32 = jnp.float32
BF16 = jnp.bfloat16
NT = (((1,), (1,)), ((), ()))
TN = (((0,), (0,)), ((), ()))


def gelu_pair(inputs):
    inner = ROOT_COEF * (inputs + CUBIC_COEF * inputs * inputs * inputs)
    tangent = jnp.tanh(inner)
    act_value = 0.5 * inputs * (1.0 + tangent)
    act_slope = 0.5 * (1.0 + tangent) + 0.5 * inputs * (1.0 - tangent * tangent) * ROOT_COEF * (
        1.0 + 3.0 * CUBIC_COEF * inputs * inputs
    )
    return (act_value, act_slope)


def iota(shape, dim):
    return lax.broadcasted_iota(jnp.int32, shape, dim)


def kernel(
    ids_any, tok_any, cot_any, win_any, wout_any, ws_any, hs_any,
    raw_in, raw_out, factors,
    ids_ref, tok_ref, cot_ref, win_ref, wout_ref, ws_ref, hs_ref,
    chunk_s, chunk_r, xall, part_s, relay_r, next_r, pair_r, far_r, work, acc, slope, hp, gin, gout,
    lane_in, lane_out, stat_h, stat_w, norm_g, norm_f, factor_own,
    a2a_ss, a2a_rs, ring_ss, ring_rs, rel_ss, rel_rs, nex_ss, nex_rs, par_ss, par_rs, far_ss, far_rs, ag_ss, ag_rs,
    sh_ss, sh_rs, sw_ss, sw_rs, ng_ss, ng_rs, nf_ss, nf_rs,
    load_sem, save_sem,
):
    p = lax.axis_index("expert")
    f = lax.axis_index("ffn")
    e = p // GROUP
    i = p % GROUP
    y = f // 2
    core = f % 2

    def turn(value, n):
        return lax.rem(value, n)

    def flip(value, mask):
        for bit in (1, 2, 4):
            if mask & bit:
                value = value + bit * (1 - 2 * turn(value // bit, 2))
        return value

    def xor(*values):
        total = 0
        for bit in (1, 2, 4):
            total = total + bit * turn(sum(value // bit for value in values), 2)
        return total

    turned = core * 4 + y
    mine = xor(turned, i, e)

    def label(m):
        return flip(mine, m ^ 6)

    def over(d):
        return flip(mine, (d % 2) * 4 + d // 2)

    def place(m):
        return (e * GROUP + flip(i, m), f)

    def side(d):
        return (p, flip(f, d))

    loads = [
        pltpu.make_async_copy(source, here, load_sem.at[index])
        for index, (source, here) in enumerate((
            (ids_any, ids_ref), (tok_any, tok_ref), (cot_any, cot_ref), (win_any, win_ref),
            (wout_any, wout_ref), (ws_any, ws_ref), (hs_any, hs_ref),
        ))
    ]
    barrier = pltpu.get_barrier_semaphore()
    for q in range(EXPERTS):
        source = q * GROUP + mine

        @pl.when(source != p)
        def _():
            pl.semaphore_signal(barrier, inc=1, device_id=(source, f), device_id_type=MESH)

    for k in range(1, GROUP):
        pl.semaphore_signal(
            barrier, inc=1, device_id=(e * GROUP + turn(i + k, GROUP), f), device_id_type=MESH
        )
        pl.semaphore_signal(barrier, inc=1, device_id=(p, turn(f + k, FFN)), device_id_type=MESH)

    for load in loads:
        load.start()

    loads[0].wait()
    ids = ids_ref[...]
    onehot = iota((EXPERTS, TOK), 0) == ids
    earlier = jnp.where(iota((TOK, TOK), 0) < iota((TOK, TOK), 1), 1.0, 0.0).astype(BF16)
    before = jnp.dot(
        jnp.where(onehot, 1.0, 0.0).astype(BF16), earlier, preferred_element_type=F32
    )
    slot = jnp.sum(jnp.where(onehot, before, 0.0), axis=0, keepdims=True).astype(jnp.int32)
    pieces_row = iota((SEND, PIECES * TOK), 0) - CAP * (iota((SEND, PIECES * TOK), 1) // TOK)

    def routed(a, expert):
        target = expert * GROUP + xor(turned, expert, i)
        copy = pltpu.make_async_remote_copy(
            src_ref=chunk_s.at[a, expert], dst_ref=chunk_r.at[a, e],
            send_sem=a2a_ss.at[a, expert], recv_sem=a2a_rs.at[a, e],
            device_id=(target, f), device_id_type=MESH,
        )
        return target, copy

    def send(a, expert):
        target, copy = routed(a, expert)

        @pl.when(target != p)
        def _():
            copy.start()

        @pl.when(target == p)
        def _():
            chunk_r[a, e] = chunk_s[a, e]

    def route(a, ref):
        loads[1 + a].wait()
        for expert in range(EXPERTS):
            spot = jnp.where(ids == expert, slot, -ROWS * 2)
            spot = jnp.concatenate([spot] * PIECES, axis=1)
            select = jnp.where(pieces_row == spot, 1.0, 0.0).astype(BF16)
            offset = xor(turned, expert, i) * BLK
            parts = [
                ref[:, pl.ds(pl.multiple_of(offset + g * 128, 128), 128)] for g in range(PIECES)
            ]
            chunk_s[a, expert] = jnp.dot(
                select, jnp.concatenate(parts, axis=0), preferred_element_type=F32
            ).astype(BF16)
            if not a and not expert:
                pl.semaphore_wait(
                    barrier, EXPERTS + 2 * (GROUP - 1) - jnp.where(mine == i, 1, 0)
                )
            if expert:
                send(a, expert - 1)
        send(a, EXPERTS - 1)

    def arrived(a):
        for q in range(EXPERTS):
            @pl.when(q * GROUP + mine != p)
            def _():
                pltpu.make_async_remote_copy(
                    src_ref=chunk_s.at[a, q], dst_ref=chunk_r.at[a, q],
                    send_sem=a2a_ss.at[a, q], recv_sem=a2a_rs.at[a, q],
                    device_id=(p, f), device_id_type=MESH,
                ).wait_recv()

    def unpack(a):
        received = chunk_r[a].reshape(EXPERTS * SEND, 128)
        row_of = iota((ROWS, EXPERTS * SEND), 0)
        source_of = lax.shift_right_logical(row_of * 3277, 16)
        gap = iota((ROWS, EXPERTS * SEND), 1) - (SEND - CAP) * source_of - row_of
        for piece in range(PIECES):
            select = jnp.where(gap == CAP * piece, 1.0, 0.0).astype(BF16)
            xall[a, mine, :, piece * 128 : (piece + 1) * 128] = jnp.dot(
                select, received, preferred_element_type=F32
            ).astype(BF16)

    def ring(a, chunk, start, size, device, index):
        rows = pl.ds(start, size)
        return pltpu.make_async_remote_copy(
            src_ref=xall.at[a, chunk, rows], dst_ref=xall.at[a, chunk, rows],
            send_sem=ring_ss.at[a, index], recv_sem=ring_rs.at[a, index],
            device_id=device, device_id_type=MESH,
        )

    half = ROWS // 2
    sent = []

    def go(copy):
        copy.start()
        sent.append(copy)

    def partial(a, m):
        x = xall[a, label(m)]
        if a:
            return lax.dot_general(x, wout_ref[...], NT, preferred_element_type=F32)
        return jnp.dot(x, win_ref[...], preferred_element_type=F32)

    def relay(a, z, h):
        return pltpu.make_async_remote_copy(
            src_ref=part_s.at[a, 2 + 4 * z, pl.ds(h * half, half)], dst_ref=relay_r.at[a, z, h],
            send_sem=rel_ss.at[a, 2 * z + h], recv_sem=rel_rs.at[a, 2 * z + h],
            device_id=place(1 + 2 * h), device_id_type=MESH,
        )

    def along_x(a, z, h):
        return pltpu.make_async_remote_copy(
            src_ref=part_s.at[a, 4 * z + 3 - 2 * h], dst_ref=next_r.at[a, z, h],
            send_sem=nex_ss.at[a, 2 * z + h], recv_sem=nex_rs.at[a, 2 * z + h],
            device_id=place(3 - 2 * h), device_id_type=MESH,
        )

    def along_z(a):
        return pltpu.make_async_remote_copy(
            src_ref=part_s.at[a, 4], dst_ref=pair_r.at[a],
            send_sem=par_ss.at[a], recv_sem=par_rs.at[a],
            device_id=place(4), device_id_type=MESH,
        )

    def far_z():
        return pltpu.make_async_remote_copy(
            src_ref=part_s.at[1, 6], dst_ref=far_r,
            send_sem=far_ss.at[0], recv_sem=far_rs.at[0],
            device_id=place(4), device_id_type=MESH,
        )

    def far(a, z):
        part_s[a, 2 + 4 * z] = partial(a, 2 + 4 * z).astype(BF16)
        go(relay(a, z, 0))
        go(relay(a, z, 1))

    def near(a, z):
        for h in (0, 1):
            work[h] = partial(a, 4 * z + 3 - 2 * h)
        for h in (0, 1):
            m = 4 * z + 3 - 2 * h
            if a and z:
                part_s[a, m] = work[h].astype(BF16)
                go(along_x(a, z, h))
                continue
            relay(a, z, h).wait_recv()
            met, other = pl.ds(h * half, half), pl.ds((1 - h) * half, half)
            part_s[a, m, other] = work[h, other].astype(BF16)
            part_s[a, m, met] = (work[h, met] + relay_r[a, z, h].astype(F32)).astype(BF16)
            go(along_x(a, z, h))

    def ring_open(a):
        go(ring(a, mine, 0, ROWS, side(2), 0))
        go(ring(a, mine, 0, ROWS, side(6), 1))
        go(ring(a, mine, 0, ROWS, side(1), 2))

    def ring_pass(a):
        ring(a, over(2), 0, ROWS, side(2), 0).wait_recv()
        go(ring(a, over(2), 0, half, side(6), 3))
        go(ring(a, over(2), 0, ROWS, side(1), 5))
        ring(a, over(6), 0, ROWS, side(6), 1).wait_recv()
        go(ring(a, over(6), half, half, side(2), 4))
        go(ring(a, over(6), 0, ROWS, side(1), 6))

    def ring_halves(a):
        ring(a, over(4), 0, half, side(6), 3).wait_recv()
        go(ring(a, over(4), 0, half, side(1), 7))
        ring(a, over(4), half, half, side(2), 4).wait_recv()
        go(ring(a, over(4), half, half, side(1), 8))

    def far_pair(a):
        ring(a, over(1), 0, ROWS, side(1), 2).wait_recv()
        far(a, 0)

    def near_pair(a):
        ring(a, over(3), 0, ROWS, side(1), 5).wait_recv()
        ring(a, over(7), 0, ROWS, side(1), 6).wait_recv()
        near(a, 0)

    def own_column(a):
        acc[a, 1] = partial(a, 4)
        ring(a, over(5), 0, half, side(1), 7).wait_recv()
        ring(a, over(5), half, half, side(1), 8).wait_recv()
        acc[a, 0] = partial(a, 0)

    def sum_x(a, z):
        along_x(a, z, 0).wait_recv()
        along_x(a, z, 1).wait_recv()
        total = acc[a, z] + next_r[a, z, 0].astype(F32) + next_r[a, z, 1].astype(F32)
        if z:
            part_s[a, 4] = total.astype(BF16)
            go(along_z(a))
        else:
            acc[a, 0] = total

    route(0, tok_ref)
    route(1, cot_ref)
    arrived(0)
    unpack(0)
    ring_open(0)
    for load in loads[3:]:
        load.wait()
    far(0, 1)
    far_pair(0)
    ring_pass(0)
    near(0, 1)
    arrived(1)
    unpack(1)
    ring_open(1)
    part_s[1, 6] = partial(1, 6).astype(BF16)
    go(far_z())
    near_pair(0)
    ring_halves(0)
    own_column(0)
    sum_x(0, 1)
    ring(1, over(1), 0, ROWS, side(1), 2).wait_recv()
    work[0] = partial(1, 2)
    ring_pass(1)
    far_z().wait_recv()
    part_s[1, 2] = (work[0] + far_r[...].astype(F32)).astype(BF16)
    go(relay(1, 0, 0))
    go(relay(1, 0, 1))
    near(1, 1)
    ring_halves(1)
    near_pair(1)
    own_column(1)
    sum_x(0, 0)
    along_z(0).wait_recv()

    owned = label(0)

    def activate(block, carry):
        rows = pl.ds(pl.multiple_of(block * 16, 16), 16)
        act_value, act_slope = gelu_pair(acc[0, 0, rows, :] + pair_r[0, rows, :].astype(F32))
        hp[0, owned, rows, :] = act_value.astype(BF16)
        slope[rows, :] = act_slope
        return carry

    def backward(block, carry):
        rows = pl.ds(pl.multiple_of(block * 16, 16), 16)
        back = acc[1, 0, rows, :] + pair_r[1, rows, :].astype(F32)
        hp[1, owned, rows, :] = (back * slope[rows, :]).astype(BF16)
        return carry

    def spread(a, m, start, size, to, index):
        rows = pl.ds(start, size)
        return pltpu.make_async_remote_copy(
            src_ref=hp.at[a, label(m), rows], dst_ref=hp.at[a, label(m), rows],
            send_sem=ag_ss.at[a, index], recv_sem=ag_rs.at[a, index],
            device_id=place(to), device_id_type=MESH,
        )

    def open_spread(a):
        go(spread(a, 0, 0, ROWS, 4, 0))
        go(spread(a, 0, 0, ROWS, 1, 1))
        go(spread(a, 0, 0, ROWS, 3, 2))

    def pass_pair(a):
        spread(a, 4, 0, ROWS, 4, 0).wait_recv()
        go(spread(a, 4, 0, ROWS, 1, 3))
        go(spread(a, 4, 0, ROWS, 3, 4))

    def pass_next(a):
        spread(a, 1, 0, ROWS, 1, 1).wait_recv()
        go(spread(a, 1, 0, half, 3, 5))
        spread(a, 3, 0, ROWS, 3, 2).wait_recv()
        go(spread(a, 3, half, half, 1, 6))

    def wait_far(a):
        spread(a, 2, 0, half, 3, 5).wait_recv()
        spread(a, 2, half, half, 1, 6).wait_recv()

    def pass_pair_next(a):
        spread(a, 5, 0, ROWS, 1, 3).wait_recv()
        go(spread(a, 5, 0, half, 3, 7))
        spread(a, 7, 0, ROWS, 3, 4).wait_recv()
        go(spread(a, 7, half, half, 1, 8))

    def wait_pair_far(a):
        spread(a, 6, 0, half, 3, 7).wait_recv()
        spread(a, 6, half, half, 1, 8).wait_recv()

    def grads(a, m, first=False):
        c = label(m)
        if a:
            add, total = lax.dot_general(
                xall[0, c], hp[1, c], TN, preferred_element_type=F32
            ), gin
        else:
            add, total = lax.dot_general(
                hp[0, c], xall[1, c], TN, preferred_element_type=F32
            ), gout
        if first:
            total[...] = add
        else:
            total[...] += add

    lax.fori_loop(0, ROWS // 16, activate, 0)
    open_spread(0)
    sum_x(1, 1)
    sum_x(1, 0)
    along_z(1).wait_recv()
    lax.fori_loop(0, ROWS // 16, backward, 0)
    open_spread(1)
    grads(0, 0, True)
    spread(0, 1, 0, ROWS, 1, 1).wait_recv()
    go(spread(0, 1, 0, half, 3, 5))
    spread(0, 3, 0, ROWS, 3, 2).wait_recv()
    go(spread(0, 3, half, half, 1, 6))
    go(spread(0, 1, 0, ROWS, 4, 3))
    go(spread(0, 3, 0, ROWS, 4, 4))
    grads(0, 1)
    grads(0, 3)
    spread(0, 4, 0, ROWS, 4, 0).wait_recv()
    grads(0, 4)
    pass_pair(1)
    pass_next(1)
    wait_far(0)
    go(spread(0, 2, 0, ROWS, 4, 7))
    grads(0, 2)
    grads(1, 0, True)
    grads(1, 4)
    grads(1, 1)
    grads(1, 3)
    spread(0, 5, 0, ROWS, 4, 3).wait_recv()
    grads(0, 5)
    pass_pair_next(1)
    grads(1, 5)
    grads(1, 7)
    spread(0, 7, 0, ROWS, 4, 4).wait_recv()
    grads(0, 7)
    wait_far(1)
    grads(1, 2)
    spread(0, 6, 0, ROWS, 4, 7).wait_recv()
    grads(0, 6)

    def squares(ref, lanes, width, rows):
        def step(block, total):
            here = pl.ds(pl.multiple_of(block * 64, 64), 64)
            folded, sums = None, []
            for g in range(width // 128):
                value = ref[here, g * 128 : (g + 1) * 128]
                value = value * value + EPS_ONE
                folded = value if folded is None else folded + value
                sums.append(jnp.sum(value.reshape(8, 8, 128), axis=0))
            lanes[here, :] = folded
            return total + jnp.concatenate(sums, axis=1)

        total = lax.fori_loop(0, rows // 64, step, jnp.zeros((8, width), F32))
        return jnp.sum(total, axis=0, keepdims=True), jnp.sum(lanes[...].T, axis=0, keepdims=True)

    hidden_prev = hs_ref[:, pl.ds(e, 1), :]
    width_prev = ws_ref[:, pl.ds(e, 1), pl.ds(pl.multiple_of(i * BLK, BLK), BLK)]

    def exchange(at, own, ssem, rsem, device):
        copies = []
        for k in range(1, 8):
            d = turn(own + k, 8)
            copies.append((
                pltpu.make_async_remote_copy(
                    src_ref=at(own), dst_ref=at(own),
                    send_sem=ssem(d), recv_sem=rsem(own),
                    device_id=device(d), device_id_type=MESH,
                ),
                pltpu.make_async_remote_copy(
                    src_ref=at(d), dst_ref=at(d),
                    send_sem=ssem(d), recv_sem=rsem(d),
                    device_id=device(d), device_id_type=MESH,
                ),
            ))
        return copies

    def in_group(d):
        return (e * GROUP + d, f)

    def in_ffn(d):
        return (p, d)

    def both(a):
        return exchange(
            lambda d: stat_h.at[a, d], i, lambda d: sh_ss.at[a, d], lambda d: sh_rs.at[a, d],
            in_group,
        ) + exchange(
            lambda d: stat_w.at[a, d], f, lambda d: sw_ss.at[a, d], lambda d: sw_rs.at[a, d],
            in_ffn,
        )

    stats = [both(0), both(1)]

    cols_out, rows_out = squares(gout, lane_out, BLK, HID)
    hidden_sum = jnp.sum(hidden_prev[1], axis=1, keepdims=True)
    stat_h[0, i] = jnp.broadcast_to(rows_out, (8, HID))
    stat_w[0, f] = jnp.concatenate([cols_out, jnp.broadcast_to(hidden_sum, (7, BLK))], axis=0)
    for start, _ in stats[0]:
        start.start()

    wait_pair_far(1)
    grads(1, 6)
    cols_in, rows_in = squares(gin, lane_in, HID, BLK)
    stat_h[1, i] = jnp.broadcast_to(cols_in, (8, HID))
    stat_w[1, f] = jnp.broadcast_to(rows_in, (8, BLK))
    for start, _ in stats[1]:
        start.start()

    def scaled(ref, lanes, scale, width, rows):
        def step(block, total):
            here = pl.ds(pl.multiple_of(block * 64, 64), 64)
            factor = lanes[here, :]
            for g in range(width // 128):
                cols = slice(g * 128, (g + 1) * 128)
                value = ref[here, cols] * factor * scale[:, cols]
                ref[here, cols] = value
                total = total + jnp.sum((value * value).reshape(8, 8, 128), axis=0)
            return total

        total = lax.fori_loop(0, rows // 64, step, jnp.zeros((8, 128), F32))
        return jnp.sum(total, axis=0, keepdims=True)

    for _, arrival in stats[0]:
        arrival.wait_recv()
    sum_out = jnp.sum(stat_w[0], axis=0)
    rows_out = DECAY_RATE * hidden_prev[1] + (1.0 - DECAY_RATE) * (
        jnp.sum(stat_h[0], axis=0)[0:1] / D
    )
    cols_out = DECAY_RATE * width_prev[1] + (1.0 - DECAY_RATE) * sum_out[0:1] / FF
    lane_out[...] = jnp.broadcast_to(lax.rsqrt(rows_out), (128, HID)).T
    norm_out = scaled(gout, lane_out, lax.rsqrt(cols_out), BLK, HID)
    save_out = pltpu.make_async_copy(gout, raw_out, save_sem.at[0])
    save_out.start()

    for _, arrival in stats[1]:
        arrival.wait_recv()
    sum_in = jnp.sum(stat_w[1], axis=0)
    cols_in = DECAY_RATE * hidden_prev[0] + (1.0 - DECAY_RATE) * (
        jnp.sum(stat_h[1], axis=0)[0:1] / D
    )
    rows_in = DECAY_RATE * width_prev[0] + (1.0 - DECAY_RATE) * sum_in[0:1] / FF
    lane_in[...] = jnp.broadcast_to(lax.rsqrt(rows_in), (128, BLK)).T
    norm_in = scaled(gin, lane_in, lax.rsqrt(cols_in), HID, BLK)
    save_in = pltpu.make_async_copy(gin, raw_in, save_sem.at[1])
    save_in.start()

    def fold(row):
        total = row[:, :128]
        for g in range(1, row.shape[1] // 128):
            total = total + row[:, g * 128 : (g + 1) * 128]
        return total

    norm_g[i] = jnp.concatenate(
        [norm_in, norm_out, fold(sum_in[0:1]), fold(sum_out[0:1]), jnp.zeros((4, 128), F32)], axis=0
    )
    group_norms = exchange(
        lambda d: norm_g.at[d], i, lambda d: ng_ss.at[d], lambda d: ng_rs.at[d], in_group
    )
    for start, _ in group_norms:
        start.start()
    for _, arrival in group_norms:
        arrival.wait_recv()
    group_sum = jnp.sum(norm_g[...], axis=0)
    norm_f[f] = group_sum
    ffn_norms = exchange(
        lambda d: norm_f.at[d], f, lambda d: nf_ss.at[d], lambda d: nf_rs.at[d], in_ffn
    )
    for start, _ in ffn_norms:
        start.start()
    for _, arrival in ffn_norms:
        arrival.wait_recv()
    norm_sum = jnp.sum(jnp.sum(norm_f[...], axis=0), axis=1, keepdims=True)
    totals = jnp.sum(group_sum, axis=1, keepdims=True)

    whole_count = float(D) * float(FF)
    width_mean = jnp.sum(ws_ref[0, pl.ds(e, 1), :], axis=1, keepdims=True) / D
    mean_in = DECAY_RATE * width_mean + (1.0 - DECAY_RATE) * totals[2:3] / whole_count
    mean_out = (
        DECAY_RATE * sum_out[1:2, 0:1] / FF + (1.0 - DECAY_RATE) * totals[3:4] / whole_count
    )
    def last_factor(mean, norm):
        return jnp.sqrt(mean) / jnp.maximum(1.0, jnp.sqrt(mean * (norm / whole_count)))

    factor_own[...] = jnp.concatenate(
        [
            jnp.broadcast_to(last_factor(mean_in, norm_sum[0:1]), (4, 128)),
            jnp.broadcast_to(last_factor(mean_out, norm_sum[1:2]), (4, 128)),
        ],
        axis=0,
    )
    save_factors = pltpu.make_async_copy(factor_own, factors, save_sem.at[2])
    save_factors.start()

    save_in.wait()
    save_out.wait()
    save_factors.wait()
    for a in range(2):
        for q in range(EXPERTS):
            target, copy = routed(a, q)

            @pl.when(target != p)
            def _():
                copy.wait_send()

    for copy in sent:
        copy.wait_send()
    for start, _ in stats[0] + stats[1] + group_norms + ffn_norms:
        start.wait_send()


def finish(
    raw_in, raw_out, factors, update_in, update_out,
    in_f32, out_f32, in_bf16, out_bf16, factor_own, load_sem, save_sem,
):
    first = pltpu.make_async_copy(factors, factor_own, load_sem.at[2 * SPLIT])
    first.start()
    parts = []
    for k in range(SPLIT):
        for j, (raw, held, done, update) in enumerate((
            (raw_in, in_f32, in_bf16, update_in), (raw_out, out_f32, out_bf16, update_out)
        )):
            rows = raw.shape[0] // SPLIT
            here = pl.ds(k * rows, rows)
            load = pltpu.make_async_copy(raw.at[here], held.at[here], load_sem.at[2 * k + j])
            load.start()
            save = pltpu.make_async_copy(done.at[here], update.at[here], save_sem.at[2 * k + j])
            parts.append((4 * j, here, held, done, load, save))
    first.wait()
    for row, here, held, done, load, save in parts:
        factor = factor_own[row : row + 1, :]
        load.wait()
        for g in range(held.shape[1] // 128):
            cols = slice(g * 128, (g + 1) * 128)
            done[here, cols] = (held[here, cols] * factor).astype(BF16)
        save.start()
    for _, _, _, _, _, save in parts:
        save.wait()


def shards(tokens, cotangent, expert_ids, in_weight, out_weight, width_states, hidden_states):
    anywhere = pl.BlockSpec(memory_space=pl.ANY)

    def dma(*shape):
        return pltpu.SemaphoreType.DMA(shape)

    operands = (
        expert_ids.reshape(1, TOK), tokens, cotangent, in_weight[0], out_weight[0],
        width_states, hidden_states,
    )
    raw_in, raw_out, factors = pl.pallas_call(
        kernel,
        out_shape=(
            jax.ShapeDtypeStruct((BLK, HID), F32),
            jax.ShapeDtypeStruct((HID, BLK), F32),
            jax.ShapeDtypeStruct((8, 128), F32),
        ),
        in_specs=[anywhere] * 7,
        out_specs=(anywhere, anywhere, anywhere),
        scratch_shapes=[pltpu.VMEM(value.shape, value.dtype) for value in operands]
        + [
            pltpu.VMEM((2, EXPERTS, SEND, 128), BF16),
            pltpu.VMEM((2, EXPERTS, SEND, 128), BF16),
            pltpu.VMEM((2, GROUP, ROWS, BLK), BF16),
            pltpu.VMEM((2, GROUP, ROWS, HID), BF16),
            pltpu.VMEM((2, 2, 2, ROWS // 2, HID), BF16),
            pltpu.VMEM((2, 2, 2, ROWS, HID), BF16),
            pltpu.VMEM((2, ROWS, HID), BF16),
            pltpu.VMEM((ROWS, HID), BF16),
            pltpu.VMEM((2, ROWS, HID), F32),
            pltpu.VMEM((2, 2, ROWS, HID), F32),
            pltpu.VMEM((ROWS, HID), F32),
            pltpu.VMEM((2, GROUP, ROWS, HID), BF16),
            pltpu.VMEM((BLK, HID), F32),
            pltpu.VMEM((HID, BLK), F32),
            pltpu.VMEM((BLK, 128), F32),
            pltpu.VMEM((HID, 128), F32),
            pltpu.VMEM((2, GROUP, 8, HID), F32),
            pltpu.VMEM((2, FFN, 8, BLK), F32),
            pltpu.VMEM((GROUP, 8, 128), F32),
            pltpu.VMEM((FFN, 8, 128), F32),
            pltpu.VMEM((8, 128), F32),
            dma(2, 8), dma(2, 8), dma(2, 9), dma(2, 9), dma(2, 4), dma(2, 4), dma(2, 4),
            dma(2, 4), dma(2), dma(2), dma(1), dma(1), dma(2, 9), dma(2, 9),
            dma(2, 8), dma(2, 8), dma(2, 8), dma(2, 8), dma(8), dma(8), dma(8), dma(8),
            dma(7), dma(3),
        ],
        compiler_params=pltpu.CompilerParams(
            collective_id=0, has_side_effects=True, vmem_limit_bytes=56 * 1024 * 1024
        ),
        name="switch_update",
    )(*operands)
    update_in, update_out = pl.pallas_call(
        finish,
        out_shape=(
            jax.ShapeDtypeStruct((BLK, HID), BF16),
            jax.ShapeDtypeStruct((HID, BLK), BF16),
        ),
        in_specs=[anywhere] * 3,
        out_specs=(anywhere, anywhere),
        scratch_shapes=[
            pltpu.VMEM((BLK, HID), F32), pltpu.VMEM((HID, BLK), F32),
            pltpu.VMEM((BLK, HID), BF16), pltpu.VMEM((HID, BLK), BF16),
            pltpu.VMEM((8, 128), F32), dma(2 * SPLIT + 1), dma(2 * SPLIT),
        ],
        compiler_params=pltpu.CompilerParams(vmem_limit_bytes=56 * 1024 * 1024),
        name="last_scaling",
    )(raw_in, raw_out, factors)
    return (update_in[None], update_out[None])


def solution(mesh):
    return jax.shard_map(
        shards,
        mesh=mesh,
        in_specs=(
            P("expert", None),
            P("expert", None),
            P("expert", None),
            P("expert", None, "ffn"),
            P("expert", "ffn", None),
            P(),
            P(None, None, "ffn"),
        ),
        out_specs=(P("expert", None, "ffn"), P("expert", "ffn", None)),
        check_vma=False,
    )
```

```python
import math

import jax
import jax.numpy as jnp
from jax import lax
from jax.experimental import pallas as pl
from jax.experimental.pallas import tpu as pltpu
from jax.sharding import PartitionSpec as P

D = 4096
FF = 5120
GROUP = 8
EXPERTS = 8
FFN = 8
CAP = 20
BLK = D // GROUP
HID = FF // FFN
TOK = 128
ROWS = GROUP * CAP
PIECES = BLK // 128
SEND = PIECES * CAP
SPLIT = 4
EDGE = 48

DECAY_RATE = 0.9
EPS_ONE = 1e-30
ROOT_COEF = math.sqrt(2.0 / math.pi)
CUBIC_COEF = 0.044715

MESH = pl.DeviceIdType.MESH
F32 = jnp.float32
BF16 = jnp.bfloat16
NT = (((1,), (1,)), ((), ()))
TN = (((0,), (0,)), ((), ()))


def gelu_pair(inputs):
    inner = ROOT_COEF * (inputs + CUBIC_COEF * inputs * inputs * inputs)
    tangent = jnp.tanh(inner)
    act_value = 0.5 * inputs * (1.0 + tangent)
    act_slope = 0.5 * (1.0 + tangent) + 0.5 * inputs * (1.0 - tangent * tangent) * ROOT_COEF * (
        1.0 + 3.0 * CUBIC_COEF * inputs * inputs
    )
    return (act_value, act_slope)


def iota(shape, dim):
    return lax.broadcasted_iota(jnp.int32, shape, dim)


def kernel(
    ids_any, tok_any, cot_any, win_any, wout_any, ws_any, hs_any,
    raw_in, raw_out, factors,
    ids_ref, tok_ref, cot_ref, win_ref, wout_ref, ws_ref, hs_ref,
    chunk_s, chunk_r, xall, part_s, relay_r, next_r, pair_r, far_r, work, acc, slope, hp, gin, gout,
    lane_in, lane_out, stat_h, stat_w, norm_g, norm_f, factor_own,
    a2a_ss, a2a_rs, ring_ss, ring_rs, rel_ss, rel_rs, nex_ss, nex_rs, par_ss, par_rs, far_ss, far_rs, ag_ss, ag_rs,
    sh_ss, sh_rs, sw_ss, sw_rs, norm_ss, norm_rs,
    load_sem, save_sem,
):
    p = lax.axis_index("expert")
    f = lax.axis_index("ffn")
    e = p // GROUP
    i = p % GROUP
    y = f // 2
    core = f % 2

    def turn(value, n):
        return lax.rem(value, n)

    def flip(value, mask):
        for bit in (1, 2, 4):
            if mask & bit:
                value = value + bit * (1 - 2 * turn(value // bit, 2))
        return value

    def xor(*values):
        total = 0
        for bit in (1, 2, 4):
            total = total + bit * turn(sum(value // bit for value in values), 2)
        return total

    turned = core * 4 + y
    mine = xor(turned, i, e)

    def label(m):
        return flip(mine, m ^ 6)

    def over(d):
        return flip(mine, (d % 2) * 4 + d // 2)

    def place(m):
        return (e * GROUP + flip(i, m), f)

    def side(d):
        return (p, flip(f, d))

    loads = [
        pltpu.make_async_copy(source, here, load_sem.at[index])
        for index, (source, here) in enumerate((
            (ids_any, ids_ref), (tok_any, tok_ref), (cot_any, cot_ref), (win_any, win_ref),
            (wout_any, wout_ref), (ws_any, ws_ref), (hs_any, hs_ref),
        ))
    ]
    barrier = pltpu.get_barrier_semaphore()
    for q in range(EXPERTS):
        source = q * GROUP + mine

        @pl.when(source != p)
        def _():
            pl.semaphore_signal(barrier, inc=1, device_id=(source, f), device_id_type=MESH)

    for k in range(1, GROUP):
        pl.semaphore_signal(
            barrier, inc=1, device_id=(e * GROUP + turn(i + k, GROUP), f), device_id_type=MESH
        )
        pl.semaphore_signal(barrier, inc=1, device_id=(p, turn(f + k, FFN)), device_id_type=MESH)

    for load in loads:
        load.start()

    loads[0].wait()
    ids = ids_ref[...]
    onehot = iota((EXPERTS, TOK), 0) == ids
    earlier = jnp.where(iota((TOK, TOK), 0) < iota((TOK, TOK), 1), 1.0, 0.0).astype(BF16)
    before = jnp.dot(
        jnp.where(onehot, 1.0, 0.0).astype(BF16), earlier, preferred_element_type=F32
    )
    slot = jnp.sum(jnp.where(onehot, before, 0.0), axis=0, keepdims=True).astype(jnp.int32)
    pieces_row = iota((SEND, PIECES * TOK), 0) - CAP * (iota((SEND, PIECES * TOK), 1) // TOK)

    def routed(a, expert):
        target = expert * GROUP + xor(turned, expert, i)
        copy = pltpu.make_async_remote_copy(
            src_ref=chunk_s.at[a, expert], dst_ref=chunk_r.at[a, e],
            send_sem=a2a_ss.at[a, expert], recv_sem=a2a_rs.at[a, e],
            device_id=(target, f), device_id_type=MESH,
        )
        return target, copy

    def send(a, expert):
        target, copy = routed(a, expert)

        @pl.when(target != p)
        def _():
            copy.start()

        @pl.when(target == p)
        def _():
            chunk_r[a, e] = chunk_s[a, e]

    def route(a, ref):
        loads[1 + a].wait()
        for expert in range(EXPERTS):
            spot = jnp.where(ids == expert, slot, -ROWS * 2)
            spot = jnp.concatenate([spot] * PIECES, axis=1)
            select = jnp.where(pieces_row == spot, 1.0, 0.0).astype(BF16)
            offset = xor(turned, expert, i) * BLK
            parts = [
                ref[:, pl.ds(pl.multiple_of(offset + g * 128, 128), 128)] for g in range(PIECES)
            ]
            chunk_s[a, expert] = jnp.dot(
                select, jnp.concatenate(parts, axis=0), preferred_element_type=F32
            ).astype(BF16)
            if not a and not expert:
                pl.semaphore_wait(
                    barrier, EXPERTS + 2 * (GROUP - 1) - jnp.where(mine == i, 1, 0)
                )
            if expert:
                send(a, expert - 1)
        send(a, EXPERTS - 1)

    def arrived(a):
        for q in range(EXPERTS):
            @pl.when(q * GROUP + mine != p)
            def _():
                pltpu.make_async_remote_copy(
                    src_ref=chunk_s.at[a, q], dst_ref=chunk_r.at[a, q],
                    send_sem=a2a_ss.at[a, q], recv_sem=a2a_rs.at[a, q],
                    device_id=(p, f), device_id_type=MESH,
                ).wait_recv()

    def unpack(a):
        received = chunk_r[a].reshape(EXPERTS * SEND, 128)
        row_of = iota((ROWS, EXPERTS * SEND), 0)
        source_of = lax.shift_right_logical(row_of * 3277, 16)
        gap = iota((ROWS, EXPERTS * SEND), 1) - (SEND - CAP) * source_of - row_of
        for piece in range(PIECES):
            select = jnp.where(gap == CAP * piece, 1.0, 0.0).astype(BF16)
            xall[a, mine, :, piece * 128 : (piece + 1) * 128] = jnp.dot(
                select, received, preferred_element_type=F32
            ).astype(BF16)

    def ring(a, chunk, start, size, device, index):
        rows = pl.ds(start, size)
        return pltpu.make_async_remote_copy(
            src_ref=xall.at[a, chunk, rows], dst_ref=xall.at[a, chunk, rows],
            send_sem=ring_ss.at[a, index], recv_sem=ring_rs.at[a, index],
            device_id=device, device_id_type=MESH,
        )

    half = ROWS // 2
    sent = []

    def go(copy):
        copy.start()
        sent.append(copy)

    def partial(a, m):
        x = xall[a, label(m)]
        if a:
            return lax.dot_general(x, wout_ref[...], NT, preferred_element_type=F32)
        return jnp.dot(x, win_ref[...], preferred_element_type=F32)

    def relay(a, z, h):
        return pltpu.make_async_remote_copy(
            src_ref=part_s.at[a, 2 + 4 * z, pl.ds(h * half, half)], dst_ref=relay_r.at[a, z, h],
            send_sem=rel_ss.at[a, 2 * z + h], recv_sem=rel_rs.at[a, 2 * z + h],
            device_id=place(1 + 2 * h), device_id_type=MESH,
        )

    def along_x(a, z, h):
        return pltpu.make_async_remote_copy(
            src_ref=part_s.at[a, 4 * z + 3 - 2 * h], dst_ref=next_r.at[a, z, h],
            send_sem=nex_ss.at[a, 2 * z + h], recv_sem=nex_rs.at[a, 2 * z + h],
            device_id=place(3 - 2 * h), device_id_type=MESH,
        )

    def along_z(a):
        return pltpu.make_async_remote_copy(
            src_ref=part_s.at[a, 4], dst_ref=pair_r.at[a],
            send_sem=par_ss.at[a], recv_sem=par_rs.at[a],
            device_id=place(4), device_id_type=MESH,
        )

    def far_z():
        return pltpu.make_async_remote_copy(
            src_ref=part_s.at[1, 6], dst_ref=far_r,
            send_sem=far_ss.at[0], recv_sem=far_rs.at[0],
            device_id=place(4), device_id_type=MESH,
        )

    def far(a, z):
        part_s[a, 2 + 4 * z] = partial(a, 2 + 4 * z).astype(BF16)
        go(relay(a, z, 0))
        go(relay(a, z, 1))

    def near(a, z):
        for h in (0, 1):
            work[h] = partial(a, 4 * z + 3 - 2 * h)
        for h in (0, 1):
            m = 4 * z + 3 - 2 * h
            if a and z:
                part_s[a, m] = work[h].astype(BF16)
                go(along_x(a, z, h))
                continue
            relay(a, z, h).wait_recv()
            met, other = pl.ds(h * half, half), pl.ds((1 - h) * half, half)
            part_s[a, m, other] = work[h, other].astype(BF16)
            part_s[a, m, met] = (work[h, met] + relay_r[a, z, h].astype(F32)).astype(BF16)
            along_x(a, z, h).start()
            if not a:
                sent.append(along_x(a, z, h))

    def ring_open(a):
        go(ring(a, mine, 0, ROWS, side(2), 0))
        go(ring(a, mine, 0, ROWS, side(6), 1))
        go(ring(a, mine, 0, ROWS, side(1), 2))

    def ring_pass(a):
        ring(a, over(2), 0, ROWS, side(2), 0).wait_recv()
        go(ring(a, over(2), 0, half, side(6), 3))
        go(ring(a, over(2), 0, ROWS, side(1), 5))
        ring(a, over(6), 0, ROWS, side(6), 1).wait_recv()
        go(ring(a, over(6), half, half, side(2), 4))
        go(ring(a, over(6), 0, ROWS, side(1), 6))

    def ring_halves(a):
        ring(a, over(4), 0, half, side(6), 3).wait_recv()
        go(ring(a, over(4), 0, half, side(1), 7))
        ring(a, over(4), half, half, side(2), 4).wait_recv()
        go(ring(a, over(4), half, half, side(1), 8))

    def far_pair(a):
        ring(a, over(1), 0, ROWS, side(1), 2).wait_recv()
        far(a, 0)

    def near_pair(a):
        ring(a, over(3), 0, ROWS, side(1), 5).wait_recv()
        ring(a, over(7), 0, ROWS, side(1), 6).wait_recv()
        near(a, 0)

    def own_column(a):
        acc[a, 1] = partial(a, 4)
        ring(a, over(5), 0, half, side(1), 7).wait_recv()
        ring(a, over(5), half, half, side(1), 8).wait_recv()
        acc[a, 0] = partial(a, 0)

    def sum_x(a, z):
        along_x(a, z, 0).wait_recv()
        along_x(a, z, 1).wait_recv()
        total = acc[a, z] + next_r[a, z, 0].astype(F32) + next_r[a, z, 1].astype(F32)
        if z:
            part_s[a, 4] = total.astype(BF16)
            go(along_z(a))
        else:
            acc[a, 0] = total

    route(0, tok_ref)
    route(1, cot_ref)
    arrived(0)
    unpack(0)
    ring_open(0)
    for load in loads[3:]:
        load.wait()
    far(0, 1)
    far_pair(0)
    ring_pass(0)
    near(0, 1)
    arrived(1)
    unpack(1)
    ring_open(1)
    part_s[1, 6] = partial(1, 6).astype(BF16)
    go(far_z())
    near_pair(0)
    ring_halves(0)
    own_column(0)
    sum_x(0, 1)
    ring(1, over(1), 0, ROWS, side(1), 2).wait_recv()
    work[0] = partial(1, 2)
    ring_pass(1)
    far_z().wait_recv()
    part_s[1, 2] = (work[0] + far_r[...].astype(F32)).astype(BF16)
    go(relay(1, 0, 0))
    go(relay(1, 0, 1))
    near(1, 1)
    ring_halves(1)
    near_pair(1)
    own_column(1)
    sum_x(0, 0)
    along_z(0).wait_recv()

    owned = label(0)

    def activate(block, carry):
        rows = pl.ds(pl.multiple_of(block * 16, 16), 16)
        act_value, act_slope = gelu_pair(acc[0, 0, rows, :] + pair_r[0, rows, :].astype(F32))
        hp[0, owned, rows, :] = act_value.astype(BF16)
        slope[rows, :] = act_slope
        return carry

    def backward(block, carry):
        rows = pl.ds(pl.multiple_of(block * 16, 16), 16)
        back = acc[1, 0, rows, :] + pair_r[1, rows, :].astype(F32)
        hp[1, owned, rows, :] = (back * slope[rows, :]).astype(BF16)
        return carry

    def spread(a, m, start, size, to, index):
        rows = pl.ds(start, size)
        return pltpu.make_async_remote_copy(
            src_ref=hp.at[a, label(m), rows], dst_ref=hp.at[a, label(m), rows],
            send_sem=ag_ss.at[a, index], recv_sem=ag_rs.at[a, index],
            device_id=place(to), device_id_type=MESH,
        )

    def open_spread(a):
        go(spread(a, 0, 0, ROWS, 4, 0))
        go(spread(a, 0, 0, ROWS, 1, 1))
        go(spread(a, 0, 0, ROWS, 3, 2))

    def pass_pair(a):
        spread(a, 4, 0, ROWS, 4, 0).wait_recv()
        go(spread(a, 4, 0, ROWS, 1, 3))
        go(spread(a, 4, 0, ROWS, 3, 4))

    def pass_next(a):
        spread(a, 1, 0, ROWS, 1, 1).wait_recv()
        go(spread(a, 1, 0, half, 3, 5))
        spread(a, 3, 0, ROWS, 3, 2).wait_recv()
        go(spread(a, 3, half, half, 1, 6))

    def wait_far(a):
        spread(a, 2, 0, half, 3, 5).wait_recv()
        spread(a, 2, half, half, 1, 6).wait_recv()

    def pass_pair_next(a):
        spread(a, 5, 0, ROWS, 1, 3).wait_recv()
        go(spread(a, 5, 0, half, 3, 7))
        spread(a, 7, 0, ROWS, 3, 4).wait_recv()
        go(spread(a, 7, half, half, 1, 8))

    def wait_pair_far(a):
        spread(a, 6, 0, half, 3, 7).wait_recv()
        spread(a, 6, half, half, 1, 8).wait_recv()

    def grads(a, m, first=False):
        c = label(m)
        if a:
            add, total = lax.dot_general(
                xall[0, c], hp[1, c], TN, preferred_element_type=F32
            ), gin
        else:
            add, total = lax.dot_general(
                hp[0, c], xall[1, c], TN, preferred_element_type=F32
            ), gout
        if first:
            total[...] = add
        else:
            total[...] += add

    lax.fori_loop(0, ROWS // 16, activate, 0)
    go(spread(0, 0, 0, half, 4, 0))
    sum_x(1, 1)
    along_x(1, 0, 0).wait_send()
    go(spread(0, 0, 0, ROWS, 3, 2))
    along_x(1, 0, 1).wait_send()
    go(spread(0, 0, 0, ROWS, 1, 1))
    sum_x(1, 0)
    along_z(1).wait_recv()
    lax.fori_loop(0, ROWS // 16, backward, 0)
    open_spread(1)
    grads(0, 0, True)
    spread(0, 1, 0, ROWS, 1, 1).wait_recv()
    go(spread(0, 1, 0, half, 3, 5))
    spread(0, 3, 0, ROWS, 3, 2).wait_recv()
    go(spread(0, 3, half, half, 1, 6))
    go(spread(0, 1, 0, ROWS, 4, 3))
    grads(0, 1)
    grads(0, 3)
    pass_pair(1)
    go(spread(0, 3, 0, ROWS, 4, 4))
    go(spread(0, 0, half, half, 4, 9))
    pass_next(1)
    wait_far(0)
    go(spread(0, 2, EDGE, ROWS - 2 * EDGE, 4, 10))
    grads(0, 2)
    grads(1, 0, True)
    grads(1, 4)
    grads(1, 1)
    grads(1, 3)
    spread(0, 5, 0, ROWS, 4, 3).wait_recv()
    go(spread(0, 5, 0, EDGE, 3, 7))
    grads(0, 5)
    pass_pair_next(1)
    spread(0, 7, 0, ROWS, 4, 4).wait_recv()
    go(spread(0, 7, ROWS - EDGE, EDGE, 1, 8))
    grads(1, 5)
    grads(1, 7)
    grads(0, 7)
    spread(0, 4, 0, half, 4, 0).wait_recv()
    spread(0, 4, half, half, 4, 9).wait_recv()
    grads(0, 4)
    wait_far(1)
    grads(1, 2)
    wait_pair_far(1)
    grads(1, 6)

    def squares(ref, lanes, width, rows):
        def step(block, total):
            here = pl.ds(pl.multiple_of(block * 64, 64), 64)
            folded, sums = None, []
            for g in range(width // 128):
                value = ref[here, g * 128 : (g + 1) * 128]
                value = value * value + EPS_ONE
                folded = value if folded is None else folded + value
                sums.append(jnp.sum(value.reshape(8, 8, 128), axis=0))
            lanes[here, :] = folded
            return total + jnp.concatenate(sums, axis=1)

        total = lax.fori_loop(0, rows // 64, step, jnp.zeros((8, width), F32))
        return jnp.sum(total, axis=0, keepdims=True), jnp.sum(lanes[...].T, axis=0, keepdims=True)

    hidden_prev = hs_ref[:, pl.ds(e, 1), :]
    width_prev = ws_ref[:, pl.ds(e, 1), pl.ds(pl.multiple_of(i * BLK, BLK), BLK)]

    def exchange(buf, own, ssem, rsem, device):
        starts = []
        for k in range(1, 8):
            starts.append(
                pltpu.make_async_remote_copy(
                    src_ref=buf.at[own], dst_ref=buf.at[own], send_sem=ssem, recv_sem=rsem,
                    device_id=device(turn(own + k, 8)), device_id_type=MESH,
                )
            )
        seven = buf.at[pl.ds(0, 7)]
        everything = pltpu.make_async_remote_copy(
            src_ref=seven, dst_ref=seven, send_sem=ssem, recv_sem=rsem,
            device_id=device(turn(own + 1, 8)), device_id_type=MESH,
        )
        return starts, everything

    def in_group(d):
        return (e * GROUP + d, f)

    def in_ffn(d):
        return (p, d)

    exchanges = [
        [
            exchange(stat_h.at[a], i, sh_ss.at[a], sh_rs.at[a], in_group),
            exchange(stat_w.at[a], f, sw_ss.at[a], sw_rs.at[a], in_ffn),
        ]
        for a in range(2)
    ]
    over_group = exchange(norm_g, i, norm_ss.at[0], norm_rs.at[0], in_group)
    over_ffn = exchange(norm_f, f, norm_ss.at[1], norm_rs.at[1], in_ffn)

    def begin(*several):
        for starts, _ in several:
            for start in starts:
                start.start()

    def collect(*several):
        for _, everything in several:
            everything.wait_recv()

    cols_in, rows_in = squares(gin, lane_in, HID, BLK)
    stat_h[1, i] = cols_in
    stat_w[1, f] = jnp.concatenate([rows_in, jnp.zeros((1, 128), F32)], axis=1)
    begin(*exchanges[1])

    spread(0, 6, 0, EDGE, 3, 7).wait_recv()
    spread(0, 6, EDGE, ROWS - 2 * EDGE, 4, 10).wait_recv()
    spread(0, 6, ROWS - EDGE, EDGE, 1, 8).wait_recv()
    grads(0, 6)
    cols_out, rows_out = squares(gout, lane_out, BLK, HID)
    hidden_sum = jnp.sum(hidden_prev[1], axis=1, keepdims=True)
    stat_h[0, i] = rows_out
    stat_w[0, f] = jnp.concatenate([cols_out, jnp.broadcast_to(hidden_sum, (1, 128))], axis=1)
    begin(*exchanges[0])

    def scaled(ref, lanes, scale, width, rows):
        def step(block, total):
            here = pl.ds(pl.multiple_of(block * 64, 64), 64)
            factor = lanes[here, :]
            for g in range(width // 128):
                cols = slice(g * 128, (g + 1) * 128)
                value = ref[here, cols] * factor * scale[:, cols]
                ref[here, cols] = value
                total = total + jnp.sum((value * value).reshape(8, 8, 128), axis=0)
            return total

        total = lax.fori_loop(0, rows // 64, step, jnp.zeros((8, 128), F32))
        return jnp.sum(total, axis=0, keepdims=True)

    collect(*exchanges[1])
    sum_in = jnp.sum(stat_w[1], axis=0)[:, :BLK]
    cols_in = DECAY_RATE * hidden_prev[0] + (1.0 - DECAY_RATE) * (jnp.sum(stat_h[1], axis=0) / D)
    rows_in = DECAY_RATE * width_prev[0] + (1.0 - DECAY_RATE) * sum_in / FF
    lane_in[...] = jnp.broadcast_to(lax.rsqrt(rows_in), (128, BLK)).T
    norm_in = scaled(gin, lane_in, lax.rsqrt(cols_in), HID, BLK)
    save_in = pltpu.make_async_copy(gin, raw_in, save_sem.at[1])
    save_in.start()

    collect(*exchanges[0])
    all_out = jnp.sum(stat_w[0], axis=0)
    sum_out = all_out[:, :BLK]
    rows_out = DECAY_RATE * hidden_prev[1] + (1.0 - DECAY_RATE) * (jnp.sum(stat_h[0], axis=0) / D)
    cols_out = DECAY_RATE * width_prev[1] + (1.0 - DECAY_RATE) * sum_out / FF
    lane_out[...] = jnp.broadcast_to(lax.rsqrt(rows_out), (128, HID)).T
    norm_out = scaled(gout, lane_out, lax.rsqrt(cols_out), BLK, HID)
    save_out = pltpu.make_async_copy(gout, raw_out, save_sem.at[0])
    save_out.start()

    def fold(row):
        total = row[:, :128]
        for g in range(1, row.shape[1] // 128):
            total = total + row[:, g * 128 : (g + 1) * 128]
        return total

    norm_g[i] = jnp.concatenate([norm_in, norm_out, fold(sum_in), fold(sum_out)], axis=1)
    begin(over_group)
    collect(over_group)
    group_sum = jnp.sum(norm_g[...], axis=0)
    norm_f[f] = group_sum
    begin(over_ffn)
    collect(over_ffn)
    norm_sum = jnp.sum(norm_f[...], axis=0)

    def total(row, part):
        return jnp.sum(row[:, part * 128 : (part + 1) * 128], axis=1, keepdims=True)

    whole_count = float(D) * float(FF)
    width_mean = jnp.sum(ws_ref[0, pl.ds(e, 1), :], axis=1, keepdims=True) / D
    mean_in = DECAY_RATE * width_mean + (1.0 - DECAY_RATE) * total(group_sum, 2) / whole_count
    mean_out = (
        DECAY_RATE * all_out[:, BLK : BLK + 1] / FF
        + (1.0 - DECAY_RATE) * total(group_sum, 3) / whole_count
    )
    def last_factor(mean, norm):
        return jnp.sqrt(mean) / jnp.maximum(1.0, jnp.sqrt(mean * (norm / whole_count)))

    factor_own[...] = jnp.concatenate(
        [
            jnp.broadcast_to(last_factor(mean_in, total(norm_sum, 0)), (4, 128)),
            jnp.broadcast_to(last_factor(mean_out, total(norm_sum, 1)), (4, 128)),
        ],
        axis=0,
    )
    save_factors = pltpu.make_async_copy(factor_own, factors, save_sem.at[2])
    save_factors.start()

    save_in.wait()
    save_out.wait()
    save_factors.wait()
    for a in range(2):
        for q in range(EXPERTS):
            target, copy = routed(a, q)

            @pl.when(target != p)
            def _():
                copy.wait_send()

    for copy in sent:
        copy.wait_send()
    for _, everything in exchanges[0] + exchanges[1] + [over_group, over_ffn]:
        everything.wait_send()


def finish(
    raw_in, raw_out, factors, update_in, update_out,
    in_f32, out_f32, in_bf16, out_bf16, factor_own, load_sem, save_sem,
):
    first = pltpu.make_async_copy(factors, factor_own, load_sem.at[2 * SPLIT])
    first.start()
    parts = []
    for k in range(SPLIT):
        for j, (raw, held, done, update) in enumerate((
            (raw_in, in_f32, in_bf16, update_in), (raw_out, out_f32, out_bf16, update_out)
        )):
            rows = raw.shape[0] // SPLIT
            here = pl.ds(k * rows, rows)
            load = pltpu.make_async_copy(raw.at[here], held.at[here], load_sem.at[2 * k + j])
            load.start()
            save = pltpu.make_async_copy(done.at[here], update.at[here], save_sem.at[2 * k + j])
            parts.append((4 * j, here, held, done, load, save))
    first.wait()
    for row, here, held, done, load, save in parts:
        factor = factor_own[row : row + 1, :]
        load.wait()
        for g in range(held.shape[1] // 128):
            cols = slice(g * 128, (g + 1) * 128)
            done[here, cols] = (held[here, cols] * factor).astype(BF16)
        save.start()
    for _, _, _, _, _, save in parts:
        save.wait()


def shards(tokens, cotangent, expert_ids, in_weight, out_weight, width_states, hidden_states):
    anywhere = pl.BlockSpec(memory_space=pl.ANY)

    def dma(*shape):
        return pltpu.SemaphoreType.DMA(shape)

    operands = (
        expert_ids.reshape(1, TOK), tokens, cotangent, in_weight[0], out_weight[0],
        width_states, hidden_states,
    )
    raw_in, raw_out, factors = pl.pallas_call(
        kernel,
        out_shape=(
            jax.ShapeDtypeStruct((BLK, HID), F32),
            jax.ShapeDtypeStruct((HID, BLK), F32),
            jax.ShapeDtypeStruct((8, 128), F32),
        ),
        in_specs=[anywhere] * 7,
        out_specs=(anywhere, anywhere, anywhere),
        scratch_shapes=[pltpu.VMEM(value.shape, value.dtype) for value in operands]
        + [
            pltpu.VMEM((2, EXPERTS, SEND, 128), BF16),
            pltpu.VMEM((2, EXPERTS, SEND, 128), BF16),
            pltpu.VMEM((2, GROUP, ROWS, BLK), BF16),
            pltpu.VMEM((2, GROUP, ROWS, HID), BF16),
            pltpu.VMEM((2, 2, 2, ROWS // 2, HID), BF16),
            pltpu.VMEM((2, 2, 2, ROWS, HID), BF16),
            pltpu.VMEM((2, ROWS, HID), BF16),
            pltpu.VMEM((ROWS, HID), BF16),
            pltpu.VMEM((2, ROWS, HID), F32),
            pltpu.VMEM((2, 2, ROWS, HID), F32),
            pltpu.VMEM((ROWS, HID), F32),
            pltpu.VMEM((2, GROUP, ROWS, HID), BF16),
            pltpu.VMEM((BLK, HID), F32),
            pltpu.VMEM((HID, BLK), F32),
            pltpu.VMEM((BLK, 128), F32),
            pltpu.VMEM((HID, 128), F32),
            pltpu.VMEM((2, GROUP, 1, HID), F32),
            pltpu.VMEM((2, FFN, 1, BLK + 128), F32),
            pltpu.VMEM((GROUP, 1, 512), F32),
            pltpu.VMEM((FFN, 1, 512), F32),
            pltpu.VMEM((8, 128), F32),
            dma(2, 8), dma(2, 8), dma(2, 9), dma(2, 9), dma(2, 4), dma(2, 4), dma(2, 4),
            dma(2, 4), dma(2), dma(2), dma(1), dma(1), dma(2, 11), dma(2, 11),
            dma(2), dma(2), dma(2), dma(2), dma(2), dma(2),
            dma(7), dma(3),
        ],
        compiler_params=pltpu.CompilerParams(
            collective_id=0, has_side_effects=True, vmem_limit_bytes=56 * 1024 * 1024
        ),
        name="switch_update",
    )(*operands)
    update_in, update_out = pl.pallas_call(
        finish,
        out_shape=(
            jax.ShapeDtypeStruct((BLK, HID), BF16),
            jax.ShapeDtypeStruct((HID, BLK), BF16),
        ),
        in_specs=[anywhere] * 3,
        out_specs=(anywhere, anywhere),
        scratch_shapes=[
            pltpu.VMEM((BLK, HID), F32), pltpu.VMEM((HID, BLK), F32),
            pltpu.VMEM((BLK, HID), BF16), pltpu.VMEM((HID, BLK), BF16),
            pltpu.VMEM((8, 128), F32), dma(2 * SPLIT + 1), dma(2 * SPLIT),
        ],
        compiler_params=pltpu.CompilerParams(vmem_limit_bytes=56 * 1024 * 1024),
        name="last_scaling",
    )(raw_in, raw_out, factors)
    return (update_in[None], update_out[None])


def solution(mesh):
    return jax.shard_map(
        shards,
        mesh=mesh,
        in_specs=(
            P("expert", None),
            P("expert", None),
            P("expert", None),
            P("expert", None, "ffn"),
            P("expert", "ffn", None),
            P(),
            P(None, None, "ffn"),
        ),
        out_specs=(P("expert", None, "ffn"), P("expert", "ffn", None)),
        check_vma=False,
    )
```

```python
import math

import jax
import jax.numpy as jnp
from jax import lax
from jax.experimental import pallas as pl
from jax.experimental.pallas import tpu as pltpu
from jax.sharding import PartitionSpec as P

D = 4096
FF = 5120
GROUP = 8
EXPERTS = 8
FFN = 8
CAP = 20
BLK = D // GROUP
HID = FF // FFN
TOK = 128
ROWS = GROUP * CAP
PIECES = BLK // 128
SEND = PIECES * CAP
SPLIT = 4
EDGE = 48

DECAY_RATE = 0.9
EPS_ONE = 1e-30
ROOT_COEF = math.sqrt(2.0 / math.pi)
CUBIC_COEF = 0.044715

MESH = pl.DeviceIdType.MESH
F32 = jnp.float32
BF16 = jnp.bfloat16
NT = (((1,), (1,)), ((), ()))
TN = (((0,), (0,)), ((), ()))


def gelu_pair(inputs):
    inner = ROOT_COEF * (inputs + CUBIC_COEF * inputs * inputs * inputs)
    tangent = jnp.tanh(inner)
    act_value = 0.5 * inputs * (1.0 + tangent)
    act_slope = 0.5 * (1.0 + tangent) + 0.5 * inputs * (1.0 - tangent * tangent) * ROOT_COEF * (
        1.0 + 3.0 * CUBIC_COEF * inputs * inputs
    )
    return (act_value, act_slope)


def iota(shape, dim):
    return lax.broadcasted_iota(jnp.int32, shape, dim)


def kernel(
    ids_any, tok_any, cot_any, win_any, wout_any, ws_any, hs_any,
    raw_in, raw_out, factors,
    ids_ref, tok_ref, cot_ref, win_ref, wout_ref, ws_ref, hs_ref,
    chunk_s, chunk_r, xall, part_s, relay_r, next_r, pair_r, far_r, work, acc, slope, hp, gin, gout,
    lane_in, lane_out, stat_h, stat_w, norm_g, norm_f, factor_own,
    a2a_ss, a2a_rs, ring_ss, ring_rs, rel_ss, rel_rs, nex_ss, nex_rs, par_ss, par_rs, far_ss, far_rs, ag_ss, ag_rs,
    sh_ss, sh_rs, sw_ss, sw_rs, norm_ss, norm_rs,
    load_sem, save_sem,
):
    p = lax.axis_index("expert")
    f = lax.axis_index("ffn")
    e = p // GROUP
    i = p % GROUP
    y = f // 2
    core = f % 2

    def turn(value, n):
        return lax.rem(value, n)

    def flip(value, mask):
        for bit in (1, 2, 4):
            if mask & bit:
                value = value + bit * (1 - 2 * turn(value // bit, 2))
        return value

    def xor(*values):
        total = 0
        for bit in (1, 2, 4):
            total = total + bit * turn(sum(value // bit for value in values), 2)
        return total

    turned = core * 4 + y
    mine = xor(turned, i, e)

    def label(m):
        return flip(mine, m ^ 6)

    def over(d):
        return flip(mine, (d % 2) * 4 + d // 2)

    def place(m):
        return (e * GROUP + flip(i, m), f)

    def side(d):
        return (p, flip(f, d))

    loads = [
        pltpu.make_async_copy(source, here, load_sem.at[index])
        for index, (source, here) in enumerate((
            (ids_any, ids_ref), (tok_any, tok_ref), (cot_any, cot_ref), (win_any, win_ref),
            (wout_any, wout_ref), (ws_any, ws_ref), (hs_any, hs_ref),
        ))
    ]
    loads[0].start()
    loads[1].start()
    barrier = pltpu.get_barrier_semaphore()
    for q in range(EXPERTS):
        source = q * GROUP + mine

        @pl.when(source != p)
        def _():
            pl.semaphore_signal(barrier, inc=1, device_id=(source, f), device_id_type=MESH)

    for k in range(1, GROUP):
        pl.semaphore_signal(
            barrier, inc=1, device_id=(e * GROUP + turn(i + k, GROUP), f), device_id_type=MESH
        )
        pl.semaphore_signal(barrier, inc=1, device_id=(p, turn(f + k, FFN)), device_id_type=MESH)

    for load in loads[2:]:
        load.start()

    loads[0].wait()
    ids = ids_ref[...]
    onehot = iota((EXPERTS, TOK), 0) == ids
    earlier = jnp.where(iota((TOK, TOK), 0) < iota((TOK, TOK), 1), 1.0, 0.0).astype(BF16)
    before = jnp.dot(
        jnp.where(onehot, 1.0, 0.0).astype(BF16), earlier, preferred_element_type=F32
    )
    slot = jnp.sum(jnp.where(onehot, before, 0.0), axis=0, keepdims=True).astype(jnp.int32)
    pieces_row = iota((SEND, PIECES * TOK), 0) - CAP * (iota((SEND, PIECES * TOK), 1) // TOK)

    def routed(a, expert):
        target = expert * GROUP + xor(turned, expert, i)
        copy = pltpu.make_async_remote_copy(
            src_ref=chunk_s.at[a, expert], dst_ref=chunk_r.at[a, e],
            send_sem=a2a_ss.at[a], recv_sem=a2a_rs.at[a],
            device_id=(target, f), device_id_type=MESH,
        )
        return target, copy

    def send(a, expert):
        target, copy = routed(a, expert)

        @pl.when(target != p)
        def _():
            copy.start()

        @pl.when(target == p)
        def _():
            chunk_r[a, e] = chunk_s[a, e]

    def route(a, ref):
        loads[1 + a].wait()
        for expert in range(EXPERTS):
            spot = jnp.where(ids == expert, slot, -ROWS * 2)
            spot = jnp.concatenate([spot] * PIECES, axis=1)
            select = jnp.where(pieces_row == spot, 1.0, 0.0).astype(BF16)
            offset = xor(turned, expert, i) * BLK
            parts = [
                ref[:, pl.ds(pl.multiple_of(offset + g * 128, 128), 128)] for g in range(PIECES)
            ]
            chunk_s[a, expert] = jnp.dot(
                select, jnp.concatenate(parts, axis=0), preferred_element_type=F32
            ).astype(BF16)
            if not a and not expert:
                pl.semaphore_wait(
                    barrier, EXPERTS + 2 * (GROUP - 1) - jnp.where(mine == i, 1, 0)
                )
            if expert:
                send(a, expert - 1)
        send(a, EXPERTS - 1)

    def all_routed(a, count):
        chunks = pl.ds(0, count)
        return pltpu.make_async_remote_copy(
            src_ref=chunk_s.at[a, chunks], dst_ref=chunk_r.at[a, chunks],
            send_sem=a2a_ss.at[a], recv_sem=a2a_rs.at[a],
            device_id=place(1), device_id_type=MESH,
        )

    def arrived(a):
        @pl.when(mine == i)
        def _():
            all_routed(a, EXPERTS - 1).wait_recv()

        @pl.when(mine != i)
        def _():
            all_routed(a, EXPERTS).wait_recv()

    def unpack(a):
        received = chunk_r[a].reshape(EXPERTS * SEND, 128)
        row_of = iota((ROWS, EXPERTS * SEND), 0)
        source_of = lax.shift_right_logical(row_of * 3277, 16)
        gap = iota((ROWS, EXPERTS * SEND), 1) - (SEND - CAP) * source_of - row_of
        for piece in range(PIECES):
            select = jnp.where(gap == CAP * piece, 1.0, 0.0).astype(BF16)
            xall[a, mine, :, piece * 128 : (piece + 1) * 128] = jnp.dot(
                select, received, preferred_element_type=F32
            ).astype(BF16)

    def ring(a, chunk, start, size, device, index):
        rows = pl.ds(start, size)
        return pltpu.make_async_remote_copy(
            src_ref=xall.at[a, chunk, rows], dst_ref=xall.at[a, chunk, rows],
            send_sem=ring_ss.at[a], recv_sem=ring_rs.at[a, index],
            device_id=device, device_id_type=MESH,
        )

    half = ROWS // 2
    sent = []

    def begin_copy(copy):
        copy.start()

    def go(copy):
        copy.start()
        sent.append(copy)

    def partial(a, m):
        x = xall[a, label(m)]
        if a:
            return lax.dot_general(x, wout_ref[...], NT, preferred_element_type=F32)
        return jnp.dot(x, win_ref[...], preferred_element_type=F32)

    def relay(a, z, h):
        return pltpu.make_async_remote_copy(
            src_ref=part_s.at[a, 2 + 4 * z, pl.ds(h * half, half)], dst_ref=relay_r.at[a, z, h],
            send_sem=rel_ss.at[a, 2 * z + h], recv_sem=rel_rs.at[a, 2 * z + h],
            device_id=place(1 + 2 * h), device_id_type=MESH,
        )

    def along_x(a, z, h):
        return pltpu.make_async_remote_copy(
            src_ref=part_s.at[a, 4 * z + 3 - 2 * h], dst_ref=next_r.at[a, z, h],
            send_sem=nex_ss.at[a, 2 * z + h], recv_sem=nex_rs.at[a, 2 * z + h],
            device_id=place(3 - 2 * h), device_id_type=MESH,
        )

    def along_z(a):
        return pltpu.make_async_remote_copy(
            src_ref=part_s.at[a, 4], dst_ref=pair_r.at[a],
            send_sem=par_ss.at[a], recv_sem=par_rs.at[a],
            device_id=place(4), device_id_type=MESH,
        )

    def far_z():
        return pltpu.make_async_remote_copy(
            src_ref=part_s.at[1, 6], dst_ref=far_r,
            send_sem=far_ss.at[0], recv_sem=far_rs.at[0],
            device_id=place(4), device_id_type=MESH,
        )

    def far(a, z):
        part_s[a, 2 + 4 * z] = partial(a, 2 + 4 * z).astype(BF16)
        go(relay(a, z, 0))
        go(relay(a, z, 1))

    def near(a, z):
        for h in (0, 1):
            work[h] = partial(a, 4 * z + 3 - 2 * h)
        for h in (0, 1):
            m = 4 * z + 3 - 2 * h
            if a and z:
                part_s[a, m] = work[h].astype(BF16)
                go(along_x(a, z, h))
                continue
            relay(a, z, h).wait_recv()
            met, other = pl.ds(h * half, half), pl.ds((1 - h) * half, half)
            part_s[a, m, other] = work[h, other].astype(BF16)
            part_s[a, m, met] = (work[h, met] + relay_r[a, z, h].astype(F32)).astype(BF16)
            along_x(a, z, h).start()
            if not a:
                sent.append(along_x(a, z, h))

    def ring_open(a):
        begin_copy(ring(a, mine, 0, ROWS, side(2), 0))
        begin_copy(ring(a, mine, 0, ROWS, side(6), 1))
        begin_copy(ring(a, mine, 0, ROWS, side(1), 2))

    def ring_pass(a):
        ring(a, over(2), 0, ROWS, side(2), 0).wait_recv()
        begin_copy(ring(a, over(2), 0, half, side(6), 3))
        begin_copy(ring(a, over(2), 0, ROWS, side(1), 5))
        ring(a, over(6), 0, ROWS, side(6), 1).wait_recv()
        begin_copy(ring(a, over(6), half, half, side(2), 4))
        begin_copy(ring(a, over(6), 0, ROWS, side(1), 6))

    def ring_halves(a):
        ring(a, over(4), 0, half, side(6), 3).wait_recv()
        begin_copy(ring(a, over(4), 0, half, side(1), 7))
        ring(a, over(4), half, half, side(2), 4).wait_recv()
        begin_copy(ring(a, over(4), half, half, side(1), 8))

    def far_pair(a):
        ring(a, over(1), 0, ROWS, side(1), 2).wait_recv()
        far(a, 0)

    def near_pair(a):
        ring(a, over(3), 0, ROWS, side(1), 5).wait_recv()
        ring(a, over(7), 0, ROWS, side(1), 6).wait_recv()
        near(a, 0)

    def own_column(a):
        acc[a, 1] = partial(a, 4)
        ring(a, over(5), 0, half, side(1), 7).wait_recv()
        ring(a, over(5), half, half, side(1), 8).wait_recv()
        acc[a, 0] = partial(a, 0)

    def sum_x(a, z):
        along_x(a, z, 0).wait_recv()
        along_x(a, z, 1).wait_recv()
        total = acc[a, z] + next_r[a, z, 0].astype(F32) + next_r[a, z, 1].astype(F32)
        if z:
            part_s[a, 4] = total.astype(BF16)
            go(along_z(a))
        else:
            acc[a, 0] = total

    route(0, tok_ref)
    route(1, cot_ref)
    arrived(0)
    unpack(0)
    ring_open(0)
    for load in loads[3:]:
        load.wait()
    far(0, 1)
    far_pair(0)
    ring_pass(0)
    near(0, 1)
    arrived(1)
    unpack(1)
    ring_open(1)
    part_s[1, 6] = partial(1, 6).astype(BF16)
    go(far_z())
    near_pair(0)
    ring_halves(0)
    own_column(0)
    sum_x(0, 1)
    ring(1, over(1), 0, ROWS, side(1), 2).wait_recv()
    work[0] = partial(1, 2)
    ring_pass(1)
    far_z().wait_recv()
    part_s[1, 2] = (work[0] + far_r[...].astype(F32)).astype(BF16)
    go(relay(1, 0, 0))
    go(relay(1, 0, 1))
    near(1, 1)
    ring_halves(1)
    near_pair(1)
    own_column(1)
    sum_x(0, 0)
    along_z(0).wait_recv()

    owned = label(0)

    def activate(block, carry):
        rows = pl.ds(pl.multiple_of(block * 16, 16), 16)
        act_value, act_slope = gelu_pair(acc[0, 0, rows, :] + pair_r[0, rows, :].astype(F32))
        hp[0, owned, rows, :] = act_value.astype(BF16)
        slope[rows, :] = act_slope
        return carry

    def backward(block, carry):
        rows = pl.ds(pl.multiple_of(block * 16, 16), 16)
        back = acc[1, 0, rows, :] + pair_r[1, rows, :].astype(F32)
        hp[1, owned, rows, :] = (back * slope[rows, :]).astype(BF16)
        return carry

    def spread(a, m, start, size, to, index):
        rows = pl.ds(start, size)
        return pltpu.make_async_remote_copy(
            src_ref=hp.at[a, label(m), rows], dst_ref=hp.at[a, label(m), rows],
            send_sem=ag_ss.at[a], recv_sem=ag_rs.at[a, index],
            device_id=place(to), device_id_type=MESH,
        )

    def open_spread(a):
        begin_copy(spread(a, 0, 0, ROWS, 4, 0))
        begin_copy(spread(a, 0, 0, ROWS, 1, 1))
        begin_copy(spread(a, 0, 0, ROWS, 3, 2))

    def pass_pair(a):
        spread(a, 4, 0, ROWS, 4, 0).wait_recv()
        begin_copy(spread(a, 4, 0, ROWS, 1, 3))
        begin_copy(spread(a, 4, 0, ROWS, 3, 4))

    def pass_next(a):
        spread(a, 1, 0, ROWS, 1, 1).wait_recv()
        begin_copy(spread(a, 1, 0, half, 3, 5))
        spread(a, 3, 0, ROWS, 3, 2).wait_recv()
        begin_copy(spread(a, 3, half, half, 1, 6))

    def wait_far(a):
        spread(a, 2, 0, half, 3, 5).wait_recv()
        spread(a, 2, half, half, 1, 6).wait_recv()

    def pass_pair_next(a):
        spread(a, 5, 0, ROWS, 1, 3).wait_recv()
        begin_copy(spread(a, 5, 0, half, 3, 7))
        spread(a, 7, 0, ROWS, 3, 4).wait_recv()
        begin_copy(spread(a, 7, half, half, 1, 8))

    def wait_pair_far(a):
        spread(a, 6, 0, half, 3, 7).wait_recv()
        spread(a, 6, half, half, 1, 8).wait_recv()

    def grads(a, m, first=False):
        c = label(m)
        if a:
            add, total = lax.dot_general(
                xall[0, c], hp[1, c], TN, preferred_element_type=F32
            ), gin
        else:
            add, total = lax.dot_general(
                hp[0, c], xall[1, c], TN, preferred_element_type=F32
            ), gout
        if first:
            total[...] = add
        else:
            total[...] += add

    lax.fori_loop(0, ROWS // 16, activate, 0)
    begin_copy(spread(0, 0, 0, half, 4, 0))
    sum_x(1, 1)
    along_x(1, 0, 0).wait_send()
    begin_copy(spread(0, 0, 0, ROWS, 3, 2))
    along_x(1, 0, 1).wait_send()
    begin_copy(spread(0, 0, 0, ROWS, 1, 1))
    sum_x(1, 0)
    along_z(1).wait_recv()
    lax.fori_loop(0, ROWS // 16, backward, 0)
    open_spread(1)
    grads(0, 0, True)
    spread(0, 1, 0, ROWS, 1, 1).wait_recv()
    begin_copy(spread(0, 1, 0, half, 3, 5))
    spread(0, 3, 0, ROWS, 3, 2).wait_recv()
    begin_copy(spread(0, 3, half, half, 1, 6))
    begin_copy(spread(0, 1, 0, ROWS, 4, 3))
    grads(0, 1)
    grads(0, 3)
    pass_pair(1)
    begin_copy(spread(0, 3, 0, ROWS, 4, 4))
    begin_copy(spread(0, 0, half, half, 4, 9))
    pass_next(1)
    wait_far(0)
    begin_copy(spread(0, 2, EDGE, ROWS - 2 * EDGE, 4, 10))
    grads(0, 2)
    grads(1, 0, True)
    grads(1, 4)
    grads(1, 1)
    grads(1, 3)
    spread(0, 5, 0, ROWS, 4, 3).wait_recv()
    begin_copy(spread(0, 5, 0, EDGE, 3, 7))
    grads(0, 5)
    pass_pair_next(1)
    spread(0, 7, 0, ROWS, 4, 4).wait_recv()
    begin_copy(spread(0, 7, ROWS - EDGE, EDGE, 1, 8))
    grads(1, 5)
    grads(1, 7)
    grads(0, 7)
    spread(0, 4, 0, half, 4, 0).wait_recv()
    spread(0, 4, half, half, 4, 9).wait_recv()
    grads(0, 4)
    wait_far(1)
    grads(1, 2)
    wait_pair_far(1)
    grads(1, 6)

    def squares(ref, lanes, width, rows):
        def step(block, total):
            here = pl.ds(pl.multiple_of(block * 64, 64), 64)
            folded, sums = None, []
            for g in range(width // 128):
                value = ref[here, g * 128 : (g + 1) * 128]
                value = value * value + EPS_ONE
                folded = value if folded is None else folded + value
                sums.append(jnp.sum(value.reshape(8, 8, 128), axis=0))
            lanes[here, :] = folded
            return total + jnp.concatenate(sums, axis=1)

        total = lax.fori_loop(0, rows // 64, step, jnp.zeros((8, width), F32))
        return jnp.sum(total, axis=0, keepdims=True), jnp.sum(lanes[...].T, axis=0, keepdims=True)

    hidden_prev = hs_ref[:, pl.ds(e, 1), :]
    width_prev = ws_ref[:, pl.ds(e, 1), pl.ds(pl.multiple_of(i * BLK, BLK), BLK)]

    def exchange(buf, own, ssem, rsem, device):
        starts = []
        for k in range(1, 8):
            starts.append(
                pltpu.make_async_remote_copy(
                    src_ref=buf.at[own], dst_ref=buf.at[own], send_sem=ssem, recv_sem=rsem,
                    device_id=device(turn(own + k, 8)), device_id_type=MESH,
                )
            )
        seven = buf.at[pl.ds(0, 7)]
        everything = pltpu.make_async_remote_copy(
            src_ref=seven, dst_ref=seven, send_sem=ssem, recv_sem=rsem,
            device_id=device(turn(own + 1, 8)), device_id_type=MESH,
        )
        return starts, everything

    def in_group(d):
        return (e * GROUP + d, f)

    def in_ffn(d):
        return (p, d)

    exchanges = [
        [
            exchange(stat_h.at[a], i, sh_ss.at[a], sh_rs.at[a], in_group),
            exchange(stat_w.at[a], f, sw_ss.at[a], sw_rs.at[a], in_ffn),
        ]
        for a in range(2)
    ]
    over_group = exchange(norm_g, i, norm_ss.at[0], norm_rs.at[0], in_group)
    over_ffn = exchange(norm_f, f, norm_ss.at[1], norm_rs.at[1], in_ffn)

    def begin(*several):
        for starts, _ in several:
            for start in starts:
                start.start()

    def collect(*several):
        for _, everything in several:
            everything.wait_recv()

    cols_in, rows_in = squares(gin, lane_in, HID, BLK)
    stat_h[1, i] = cols_in
    stat_w[1, f] = jnp.concatenate([rows_in, jnp.zeros((1, 128), F32)], axis=1)
    begin(*exchanges[1])

    spread(0, 6, 0, EDGE, 3, 7).wait_recv()
    spread(0, 6, EDGE, ROWS - 2 * EDGE, 4, 10).wait_recv()
    spread(0, 6, ROWS - EDGE, EDGE, 1, 8).wait_recv()
    grads(0, 6)
    cols_out, rows_out = squares(gout, lane_out, BLK, HID)
    hidden_sum = jnp.sum(hidden_prev[1], axis=1, keepdims=True)
    stat_h[0, i] = rows_out
    stat_w[0, f] = jnp.concatenate([cols_out, jnp.broadcast_to(hidden_sum, (1, 128))], axis=1)
    begin(*exchanges[0])

    def scaled(ref, lanes, scale, width, rows):
        def step(block, total):
            here = pl.ds(pl.multiple_of(block * 64, 64), 64)
            factor = lanes[here, :]
            for g in range(width // 128):
                cols = slice(g * 128, (g + 1) * 128)
                value = ref[here, cols] * factor * scale[:, cols]
                ref[here, cols] = value
                total = total + jnp.sum((value * value).reshape(8, 8, 128), axis=0)
            return total

        total = lax.fori_loop(0, rows // 64, step, jnp.zeros((8, 128), F32))
        return jnp.sum(total, axis=0, keepdims=True)

    collect(*exchanges[1])
    sum_in = jnp.sum(stat_w[1], axis=0)[:, :BLK]
    cols_in = DECAY_RATE * hidden_prev[0] + (1.0 - DECAY_RATE) * (jnp.sum(stat_h[1], axis=0) / D)
    rows_in = DECAY_RATE * width_prev[0] + (1.0 - DECAY_RATE) * sum_in / FF
    lane_in[...] = jnp.broadcast_to(lax.rsqrt(rows_in), (128, BLK)).T
    norm_in = scaled(gin, lane_in, lax.rsqrt(cols_in), HID, BLK)
    save_in = pltpu.make_async_copy(gin, raw_in, save_sem.at[1])
    save_in.start()

    collect(*exchanges[0])
    all_out = jnp.sum(stat_w[0], axis=0)
    sum_out = all_out[:, :BLK]
    rows_out = DECAY_RATE * hidden_prev[1] + (1.0 - DECAY_RATE) * (jnp.sum(stat_h[0], axis=0) / D)
    cols_out = DECAY_RATE * width_prev[1] + (1.0 - DECAY_RATE) * sum_out / FF
    lane_out[...] = jnp.broadcast_to(lax.rsqrt(rows_out), (128, HID)).T
    norm_out = scaled(gout, lane_out, lax.rsqrt(cols_out), BLK, HID)
    save_out = pltpu.make_async_copy(gout, raw_out, save_sem.at[0])
    save_out.start()

    def fold(row):
        total = row[:, :128]
        for g in range(1, row.shape[1] // 128):
            total = total + row[:, g * 128 : (g + 1) * 128]
        return total

    norm_g[i] = jnp.concatenate([norm_in, norm_out, fold(sum_in), fold(sum_out)], axis=1)
    begin(over_group)
    collect(over_group)
    group_sum = jnp.sum(norm_g[...], axis=0)
    norm_f[f] = group_sum
    begin(over_ffn)
    collect(over_ffn)
    norm_sum = jnp.sum(norm_f[...], axis=0)

    def total(row, part):
        return jnp.sum(row[:, part * 128 : (part + 1) * 128], axis=1, keepdims=True)

    whole_count = float(D) * float(FF)
    width_mean = jnp.sum(ws_ref[0, pl.ds(e, 1), :], axis=1, keepdims=True) / D
    mean_in = DECAY_RATE * width_mean + (1.0 - DECAY_RATE) * total(group_sum, 2) / whole_count
    mean_out = (
        DECAY_RATE * all_out[:, BLK : BLK + 1] / FF
        + (1.0 - DECAY_RATE) * total(group_sum, 3) / whole_count
    )
    def last_factor(mean, norm):
        return jnp.sqrt(mean) / jnp.maximum(1.0, jnp.sqrt(mean * (norm / whole_count)))

    factor_own[...] = jnp.concatenate(
        [
            jnp.broadcast_to(last_factor(mean_in, total(norm_sum, 0)), (4, 128)),
            jnp.broadcast_to(last_factor(mean_out, total(norm_sum, 1)), (4, 128)),
        ],
        axis=0,
    )
    save_factors = pltpu.make_async_copy(factor_own, factors, save_sem.at[2])
    save_factors.start()

    save_in.wait()
    save_out.wait()
    save_factors.wait()
    seven = pl.ds(0, GROUP - 1)
    for a in range(2):
        @pl.when(mine == i)
        def _():
            all_routed(a, EXPERTS - 1).wait_send()

        @pl.when(mine != i)
        def _():
            all_routed(a, EXPERTS).wait_send()

        pltpu.make_async_remote_copy(
            src_ref=xall.at[a, seven], dst_ref=xall.at[a, seven],
            send_sem=ring_ss.at[a], recv_sem=ring_rs.at[a, 0],
            device_id=side(1), device_id_type=MESH,
        ).wait_send()
        pltpu.make_async_remote_copy(
            src_ref=hp.at[a, seven], dst_ref=hp.at[a, seven],
            send_sem=ag_ss.at[a], recv_sem=ag_rs.at[a, 0],
            device_id=place(1), device_id_type=MESH,
        ).wait_send()

    for copy in sent:
        copy.wait_send()
    for _, everything in exchanges[0] + exchanges[1] + [over_group, over_ffn]:
        everything.wait_send()


def finish(
    raw_in, raw_out, factors, update_in, update_out,
    in_f32, out_f32, in_bf16, out_bf16, factor_own, load_sem, save_sem,
):
    first = pltpu.make_async_copy(factors, factor_own, load_sem.at[2 * SPLIT])
    first.start()
    parts = []
    for k in range(SPLIT):
        for j, (raw, held, done, update) in enumerate((
            (raw_in, in_f32, in_bf16, update_in), (raw_out, out_f32, out_bf16, update_out)
        )):
            rows = raw.shape[0] // SPLIT
            here = pl.ds(k * rows, rows)
            load = pltpu.make_async_copy(raw.at[here], held.at[here], load_sem.at[2 * k + j])
            load.start()
            save = pltpu.make_async_copy(done.at[here], update.at[here], save_sem.at[2 * k + j])
            parts.append((4 * j, here, held, done, load, save))
    first.wait()
    for row, here, held, done, load, save in parts:
        factor = factor_own[row : row + 1, :]
        load.wait()
        for g in range(held.shape[1] // 128):
            cols = slice(g * 128, (g + 1) * 128)
            done[here, cols] = (held[here, cols] * factor).astype(BF16)
        save.start()
    for _, _, _, _, _, save in parts:
        save.wait()


def shards(tokens, cotangent, expert_ids, in_weight, out_weight, width_states, hidden_states):
    anywhere = pl.BlockSpec(memory_space=pl.ANY)

    def dma(*shape):
        return pltpu.SemaphoreType.DMA(shape)

    operands = (
        expert_ids.reshape(1, TOK), tokens, cotangent, in_weight[0], out_weight[0],
        width_states, hidden_states,
    )
    raw_in, raw_out, factors = pl.pallas_call(
        kernel,
        out_shape=(
            jax.ShapeDtypeStruct((BLK, HID), F32),
            jax.ShapeDtypeStruct((HID, BLK), F32),
            jax.ShapeDtypeStruct((8, 128), F32),
        ),
        in_specs=[anywhere] * 7,
        out_specs=(anywhere, anywhere, anywhere),
        scratch_shapes=[pltpu.VMEM(value.shape, value.dtype) for value in operands]
        + [
            pltpu.VMEM((2, EXPERTS, SEND, 128), BF16),
            pltpu.VMEM((2, EXPERTS, SEND, 128), BF16),
            pltpu.VMEM((2, GROUP, ROWS, BLK), BF16),
            pltpu.VMEM((2, GROUP, ROWS, HID), BF16),
            pltpu.VMEM((2, 2, 2, ROWS // 2, HID), BF16),
            pltpu.VMEM((2, 2, 2, ROWS, HID), BF16),
            pltpu.VMEM((2, ROWS, HID), BF16),
            pltpu.VMEM((ROWS, HID), BF16),
            pltpu.VMEM((2, ROWS, HID), F32),
            pltpu.VMEM((2, 2, ROWS, HID), F32),
            pltpu.VMEM((ROWS, HID), F32),
            pltpu.VMEM((2, GROUP, ROWS, HID), BF16),
            pltpu.VMEM((BLK, HID), F32),
            pltpu.VMEM((HID, BLK), F32),
            pltpu.VMEM((BLK, 128), F32),
            pltpu.VMEM((HID, 128), F32),
            pltpu.VMEM((2, GROUP, 1, HID), F32),
            pltpu.VMEM((2, FFN, 1, BLK + 128), F32),
            pltpu.VMEM((GROUP, 1, 512), F32),
            pltpu.VMEM((FFN, 1, 512), F32),
            pltpu.VMEM((8, 128), F32),
            dma(2), dma(2), dma(2), dma(2, 9), dma(2, 4), dma(2, 4), dma(2, 4),
            dma(2, 4), dma(2), dma(2), dma(1), dma(1), dma(2), dma(2, 11),
            dma(2), dma(2), dma(2), dma(2), dma(2), dma(2),
            dma(7), dma(3),
        ],
        compiler_params=pltpu.CompilerParams(
            collective_id=0, has_side_effects=True, vmem_limit_bytes=56 * 1024 * 1024
        ),
        name="switch_update",
    )(*operands)
    update_in, update_out = pl.pallas_call(
        finish,
        out_shape=(
            jax.ShapeDtypeStruct((BLK, HID), BF16),
            jax.ShapeDtypeStruct((HID, BLK), BF16),
        ),
        in_specs=[anywhere] * 3,
        out_specs=(anywhere, anywhere),
        scratch_shapes=[
            pltpu.VMEM((BLK, HID), F32), pltpu.VMEM((HID, BLK), F32),
            pltpu.VMEM((BLK, HID), BF16), pltpu.VMEM((HID, BLK), BF16),
            pltpu.VMEM((8, 128), F32), dma(2 * SPLIT + 1), dma(2 * SPLIT),
        ],
        compiler_params=pltpu.CompilerParams(vmem_limit_bytes=56 * 1024 * 1024),
        name="last_scaling",
    )(raw_in, raw_out, factors)
    return (update_in[None], update_out[None])


def solution(mesh):
    return jax.shard_map(
        shards,
        mesh=mesh,
        in_specs=(
            P("expert", None),
            P("expert", None),
            P("expert", None),
            P("expert", None, "ffn"),
            P("expert", "ffn", None),
            P(),
            P(None, None, "ffn"),
        ),
        out_specs=(P("expert", None, "ffn"), P("expert", "ffn", None)),
        check_vma=False,
    )
```
